256 devices in a mesh: gx: 8 (over z), gy: 8 (over y, core), gz: 4 (over x).
Axes of the slice: x: 4, y: 4, z: 8, core: 2. Of those that a mesh axis runs over, the one named last changes fastest.
Arguments:
- acts: bfloat16 [150528, 2048], P(('gx', 'gy', 'gz')), may hold values from -24 to 24
- saved_hidden: bfloat16 [150528, 512], P(('gx', 'gy', 'gz')), as said below
- grad_out: bfloat16 [150528, 2048], P(('gx', 'gy', 'gz')), may hold values from -24 to 24
- master_reduce: float32 [2048, 512], P(('gx', 'gy', 'gz')), may hold values from -60 to 60
- master_expand: float32 [2048, 512], P(('gx', 'gy', 'gz')), may hold values from -60 to 60
- velocity_reduce: float32 [2048, 512], P(('gx', 'gy', 'gz')), may hold values from -6 to 6
- velocity_expand: float32 [2048, 512], P(('gx', 'gy', 'gz')), may hold values from -6 to 6
Outputs:
- grad_in: bfloat16 [150528, 2048], P(('gx', 'gy', 'gz'))
- new_master_reduce: float32 [2048, 512], P(('gx', 'gy', 'gz'))
- new_master_expand: float32 [2048, 512], P(('gx', 'gy', 'gz'))
- new_velocity_reduce: float32 [2048, 512], P(('gx', 'gy', 'gz'))
- new_velocity_expand: float32 [2048, 512], P(('gx', 'gy', 'gz'))
- work_reduce: bfloat16 [2048, 512], replicated
- work_expand: bfloat16 [2048, 512], replicated
The draws below stay inside these ranges and needn't reach their ends.
Inputs may be any that keep to these rules, and one draw needn't show every extreme that they name: `saved_hidden`: values are zero or positive, zero at about half of the entries.
All inputs are finite; a program needn't handle non-finite values.
Results may differ from the reference program's by a relative error of at most 0.0064.
Values may be sent and summed in bfloat16 or wider, within the bound.
A program may use at most 64 MiB of HBM per device.

```python
import jax
import jax.numpy as jnp
from jax import lax

CHANNELS = 2048
MIDDLE = 512
ROWS = 150528


def draw_saved_hidden(key, part):
    values = jax.random.normal(jax.random.fold_in(key, 11), (ROWS, MIDDLE), jnp.float32)
    return jnp.maximum(values, 0.0).astype(jnp.bfloat16)


def rising_master(key, salt):
    values = jnp.clip(jax.random.normal(jax.random.fold_in(key, salt), (CHANNELS, MIDDLE), jnp.float32), -6.0, 6.0)
    place = jnp.arange(CHANNELS, dtype=jnp.float32)[:, None] / float(max(CHANNELS - 1, 1))
    scales = 1.0 + 2.0 * place
    return values * scales


def draw_master_reduce(key, part):
    return rising_master(key, 21)


def draw_master_expand(key, part):
    return rising_master(key, 31)


def strengthened(entries, stream_key, source, target, shards_of, factor):
    owner, partner = [(jnp.arange(entries.shape[dim]) // (entries.shape[dim] // shards_of)).reshape([-1 if axis == dim else 1 for axis in range(entries.ndim)]) for dim in (source, target)]
    chosen = jax.random.permutation(stream_key, shards_of)[partner]
    strong = (owner == chosen) | (owner == (partner + shards_of // 2) % shards_of)
    return jnp.where(strong, factor * entries, entries)


def levels(key, extent, cuts, least, high):
    def one(dim, shards_of):
        steps = jax.random.uniform(jax.random.fold_in(jax.random.fold_in(key, 6), dim), (shards_of,), jnp.float32, least / len(cuts), high / len(cuts))
        return jnp.repeat(jnp.exp(steps), extent[dim] // shards_of).reshape((-1,) + (1,) * (len(extent) - dim - 1))

    level = one(*cuts[0])
    for cut in cuts[1:]:
        level = level * one(*cut)
    return level


def gaussian(rng, dims, deviation, most, cuts=(), held_as=jnp.bfloat16):
    level = levels(rng, dims, cuts, -0.22, 0.18) if cuts else 1.0
    entries = jax.random.normal(rng, dims, jnp.float32) * deviation * level
    return jnp.minimum(jnp.maximum(entries, -most), most).astype(held_as)


def gaussian_with(rng, extent, scale, most, split, heavy, held_as=jnp.bfloat16):
    drawn = scale * jax.random.normal(rng, extent, jnp.float32)
    if split:
        drawn = drawn * levels(rng, extent, split, -0.22, 0.18)
    return jnp.clip(strengthened(drawn, jax.random.fold_in(rng, 3), *heavy), -most, most).astype(held_as)


def setup_inputs(seed: int = 0) -> dict:
    key_list = jax.random.split(jax.random.key(seed), 8)
    return {
        "acts": gaussian_with(key_list[0], (ROWS, CHANNELS), 1.0, 24.0, ((0, 256),), (0, 1, 256, 6.0)),
        "saved_hidden": draw_saved_hidden(jax.random.fold_in(key_list[7], 71), 0),
        "grad_out": gaussian_with(key_list[2], (ROWS, CHANNELS), 1.0, 24.0, ((0, 256),), (0, 1, 256, 6.0)),
        "master_reduce": draw_master_reduce(jax.random.fold_in(key_list[7], 71), 0),
        "master_expand": draw_master_expand(jax.random.fold_in(key_list[7], 71), 0),
        "velocity_reduce": gaussian(key_list[5], (CHANNELS, MIDDLE), 1.0, 6.0, ((0, 256),), jnp.float32),
        "velocity_expand": gaussian(key_list[6], (CHANNELS, MIDDLE), 1.0, 6.0, ((0, 256),), jnp.float32),
    }


def layer_update(master, grads, velocity):
    wnorm = jnp.sqrt(jnp.sum(master * master))
    gnorm = jnp.sqrt(jnp.sum(grads * grads))
    trust = wnorm / (gnorm + 5e-05 * wnorm)
    new_velocity = 0.9 * velocity + trust * (grads + 5e-05 * master)
    new_master = master - 0.1 * new_velocity
    return (new_master, new_velocity, new_master.astype(jnp.bfloat16))

def reference(acts, saved_hidden, grad_out, master_reduce, master_expand, velocity_reduce, velocity_expand):
    inv_c = 1.0 / math_sqrt(CHANNELS)
    inv_m = 1.0 / math_sqrt(MIDDLE)
    cur_reduce = master_reduce.astype(jnp.bfloat16)
    cur_expand = master_expand.astype(jnp.bfloat16)
    summed = jnp.dot(grad_out, cur_expand, preferred_element_type=jnp.float32)
    grad_hidden = jnp.where(saved_hidden > 0, summed * inv_m, 0.0).astype(jnp.bfloat16)
    g_expand = lax.dot_general(grad_out, saved_hidden, (((0,), (0,)), ((), ())), preferred_element_type=jnp.float32) * inv_m
    g_reduce = lax.dot_general(acts, grad_hidden, (((0,), (0,)), ((), ())), preferred_element_type=jnp.float32) * inv_c
    back = lax.dot_general(grad_hidden, cur_reduce, (((1,), (1,)), ((), ())), preferred_element_type=jnp.float32)
    grad_in = (grad_out.astype(jnp.float32) + back * inv_c).astype(jnp.bfloat16)
    new_mr, new_vr, work_reduce = layer_update(master_reduce, g_reduce, velocity_reduce)
    new_me, new_ve, work_expand = layer_update(master_expand, g_expand, velocity_expand)
    return (grad_in, new_mr, new_me, new_vr, new_ve, work_reduce, work_expand)

def math_sqrt(value):
    return float(value) ** 0.5
```

```python
import jax
import jax.numpy as jnp
from jax import lax
from jax.experimental import pallas as pl
from jax.experimental.pallas import tpu as pltpu
from jax.sharding import PartitionSpec as P

MESH = pl.DeviceIdType.MESH
BF16 = jnp.bfloat16
F32 = jnp.float32
ROWS_SPLIT = ("gx", "gy", "gz")
NZ, NY, NX, NK = 8, 4, 4, 2
BLK = 8
SEMS = 320


class Net:
    def __init__(self, send, recv):
        self.send, self.recv, self.used = send, recv, 0

    def put(self, src, dst, peer):
        at = self.used
        self.used += 1
        copy = pltpu.make_async_remote_copy(
            src_ref=src,
            dst_ref=dst,
            send_sem=self.send.at[at],
            recv_sem=self.recv.at[at],
            device_id=peer,
            device_id_type=MESH,
        )
        copy.start()
        return copy


class Place:
    def __init__(self):
        self.z = lax.axis_index("gx")
        gy = lax.axis_index("gy")
        self.y = gy // 2
        self.k = gy % 2
        self.x = lax.axis_index("gz")
        self.gy = gy
        self.kx = self.k * NX + self.x
        self.d = 1 - 2 * self.k

    def zp(self, j):
        return {"gx": (self.z + j) % NZ}

    def yp(self, j):
        return {"gy": ((self.y + j + NY) % NY) * 2 + self.k}

    def xp(self, j):
        return {"gz": (self.x + j + NX) % NX}

    def other(self):
        return {"gy": self.gy + 1 - 2 * self.k}


class Gather:
    def __init__(self, net, me, w):
        self.net, self.me, self.w = net, me, w
        cols = w.shape[-1]
        half = cols // 2
        self.parts = (pl.ds(0, half), pl.ds(half, half))
        self.cores = []
        self.sent = []

    def put(self, ref, peer):
        copy = self.net.put(ref, ref, peer)
        self.sent.append(copy)
        return copy

    def along_z(self):
        me = self.me
        ref = self.w.at[me.z, me.y, me.kx]
        self.zs = [self.put(ref, me.zp(j)) for j in (4, 3, 5, 2, 6, 1, 7)]

    def middle(self):
        me = self.me
        for copy in self.zs:
            copy.wait_recv()
        self.mids = []
        for part, peer in zip(self.parts, (me.yp, me.xp)):
            ref = self.w.at[:, me.y, me.kx, :, part]
            self.mids.append([self.put(ref, peer(j)) for j in (2, 1, 3)])

    def slab(self, part, off):
        me = self.me
        if part == 0:
            x = (me.x + off + NX) % NX
            return self.w.at[:, :, me.k * NX + x, :, self.parts[0]]
        y = (me.y + off + NY) % NY
        return self.w.at[:, y, pl.ds(me.k * NX, NX), :, self.parts[1]]

    def peer(self, part, off):
        return self.me.xp(off) if part == 0 else self.me.yp(off)

    def core(self, part, off):
        self.cores.append(self.put(self.slab(part, off), self.me.other()))

    def large(self):
        d = self.me.d
        self.near = []
        for part in range(2):
            for copy in self.mids[part]:
                copy.wait_recv()
            ref = self.slab(part, 0)
            self.near.append((self.put(ref, self.peer(part, d)), self.put(ref, self.peer(part, -d))))
            self.core(part, 0)

    def forward(self):
        d = self.me.d
        self.far = []
        for part in range(2):
            self.near[part][0].wait_recv()
            self.far.append(self.put(self.slab(part, -d), self.peer(part, d)))
            self.core(part, -d)

    def finish(self):
        d = self.me.d
        for part in range(2):
            self.near[part][1].wait_recv()
            self.core(part, d)
        for part in range(2):
            self.far[part].wait_recv()
            self.core(part, 2)

    def arrived(self):
        for copy in self.cores:
            copy.wait_recv()

    def drain(self):
        for copy in self.sent:
            copy.wait_send()


def add_blocks(count, out, *terms):
    def step(i, carry):
        total = terms[0](i).astype(F32)
        for term in terms[1:]:
            total = total + term(i).astype(F32)
        out(i, total)
        return carry

    lax.fori_loop(0, count, step, 0)


class Scatter:
    def __init__(self, net, me, refs):
        self.net, self.me = net, me
        (self.p, self.c, self.s, self.f, self.t, self.r, self.a, self.m, self.b, self.q) = refs
        self.sent = []

    def put(self, src, dst, peer):
        copy = self.net.put(src, dst, peer)
        self.sent.append(copy)
        return copy

    def tile(self, t, value):
        half = value.shape[1] // 2
        for y in range(NY):
            for k in range(NK):
                for x in range(NX):
                    at = ((y * NK + k) * NX + x) * BLK
                    rows = value[at : at + BLK]
                    self.p[0, k, x, y * NZ + t] = rows[:, :half].astype(BF16)
                    self.p[1, k, y, x * NZ + t] = rows[:, half:].astype(BF16)

    def cores(self):
        me = self.me
        self.cs = [
            self.put(self.p.at[part, 1 - me.k], self.c.at[part], me.other()) for part in range(2)
        ]

    def peer(self, part, off):
        return self.me.xp(off) if part == 0 else self.me.yp(off)

    def index(self, part, off):
        return (self.me.x + off + NX) % NX if part == 0 else (self.me.y + off + NY) % NY

    def large(self):
        me = self.me
        d = me.d
        self.near = []
        for part in range(2):
            self.cs[part].wait_recv()
            first = self.put(self.joined(part, 2), self.f.at[part], self.peer(part, d))
            second = self.put(self.joined(part, -d), self.r.at[part, 0], self.peer(part, -d))
            self.near.append((first, second))
        for part in range(2):
            self.joined(part, d)
            self.joined(part, 0)

    def joined(self, part, off):
        me = self.me
        at = self.index(part, off)

        def out(i, total):
            self.s[part, at, pl.ds(i * 8, 8)] = total.astype(BF16)

        add_blocks(
            4,
            out,
            lambda i: self.p[part, me.k, at, pl.ds(i * 8, 8)],
            lambda i: self.c[part, at, pl.ds(i * 8, 8)],
        )
        return self.s.at[part, at]

    def forward(self):
        d = self.me.d
        self.far = []
        for part in range(2):
            self.near[part][0].wait_recv()
            at = self.index(part, d)

            def out(i, total, part=part):
                self.t[part, pl.ds(i * 8, 8)] = total.astype(BF16)

            add_blocks(
                4,
                out,
                lambda i, part=part, at=at: self.s[part, at, pl.ds(i * 8, 8)],
                lambda i, part=part: self.f[part, pl.ds(i * 8, 8)],
            )
            self.far.append(self.put(self.t.at[part], self.r.at[part, 1], self.peer(part, d)))

    def middle(self):
        me = self.me
        self.mids = []
        for part in range(2):
            self.near[part][1].wait_recv()
            self.far[part].wait_recv()
            at = self.index(part, 0)

            def out(i, total, part=part):
                self.a[part, pl.ds(i * 8, 8)] = total.astype(BF16)

            add_blocks(
                4,
                out,
                lambda i, part=part, at=at: self.s[part, at, pl.ds(i * 8, 8)],
                lambda i, part=part: self.r[part, 0, pl.ds(i * 8, 8)],
                lambda i, part=part: self.r[part, 1, pl.ds(i * 8, 8)],
            )
            copies = []
            for j in (2, 1, 3):
                to = self.index(1 - part, j)
                copies.append(
                    self.put(
                        self.a.at[part, pl.ds(to * 8, 8)],
                        self.m.at[part, j - 1],
                        self.peer(1 - part, j),
                    )
                )
            self.mids.append(copies)

    def along_z(self):
        me = self.me
        for part in range(2):
            for copy in self.mids[part]:
                copy.wait_recv()
            at = self.index(1 - part, 0)
            total = self.a[part, pl.ds(at * 8, 8)].astype(F32)
            for j in range(3):
                total = total + self.m[part, j].astype(F32)
            half = total.shape[-1]
            self.b[:, :, pl.ds(part * half, half)] = total.astype(BF16)
        self.zs = []
        for j in (4, 3, 5, 2, 6, 1, 7):
            self.zs.append(self.put(self.b.at[(me.z + j) % NZ], self.q.at[j - 1], me.zp(j)))

    def result(self):
        for copy in self.zs:
            copy.wait_recv()
        total = self.b[self.me.z].astype(F32)
        for j in range(7):
            total = total + self.q[j].astype(F32)
        return total

    def drain(self):
        for copy in self.sent:
            copy.wait_send()


class Norms:
    def __init__(self, net, me, refs):
        self.net, self.me, self.refs = net, me, refs
        self.sent = []

    def start(self, axis, tile):
        me = self.me
        ref = self.refs[axis]
        own = (me.z, me.y, me.x, me.k)[axis]
        ref[own] = tile
        peers = (
            [me.zp(j) for j in (4, 3, 5, 2, 6, 1, 7)],
            [me.yp(j) for j in (2, 1, 3)],
            [me.xp(j) for j in (2, 1, 3)],
            [me.other()],
        )[axis]
        self.flying = [self.net.put(ref.at[own], ref.at[own], peer) for peer in peers]
        self.sent += self.flying

    def finish(self, axis):
        ref = self.refs[axis]
        for copy in self.flying:
            copy.wait_recv()
        total = ref[0]
        for i in range(1, ref.shape[0]):
            total = total + ref[i]
        return total

    def drain(self):
        for copy in self.sent:
            copy.wait_send()


def fold(sq):
    lanes = sq[:, 0:128]
    for i in range(1, sq.shape[1] // 128):
        lanes = lanes + sq[:, 128 * i : 128 * (i + 1)]
    return jnp.sum(lanes, axis=0, keepdims=True)


def stat_tile(w, g):
    row = lax.broadcasted_iota(jnp.int32, (8, 128), 0)
    wrow = jnp.broadcast_to(fold(w * w), (8, 128))
    grow = jnp.broadcast_to(fold(g * g), (8, 128))
    return jnp.where(row == 0, wrow, jnp.where(row == 1, grow, 0.0))


def updated(master, grads, velocity, tile):
    wsquare = jnp.sum(tile[0:1, :], axis=1, keepdims=True)
    gsquare = jnp.sum(tile[1:2, :], axis=1, keepdims=True)
    wnorm = jnp.sqrt(wsquare)
    gnorm = jnp.sqrt(gsquare)
    trust = wnorm / (gnorm + 5e-05 * wnorm)
    new_velocity = 0.9 * velocity + trust * (grads + 5e-05 * master)
    new_master = master - 0.1 * new_velocity
    return new_master, new_velocity


def kernel(
    acts_h, hid_h, go_h, mr_h, me_h, vr_h, ve_h,
    gi_h, nmr_h, nme_h, nvr_h, nve_h, wr_h, we_h,
    acts, hid, go, small, smallout, gi, gh, acc,
    we, wr, ne, nr, flat, ge_refs, gr_refs, nz_e, nz_r,
    send, recv, load, out_sem,
):
    me = Place()
    net = Net(send, recv)
    channels = go.shape[1]
    middle = hid.shape[1]
    inv_c = 1.0 / float(channels) ** 0.5
    inv_m = 1.0 / float(middle) ** 0.5

    loads = [
        pltpu.make_async_copy(src, dst, load.at[i])
        for i, (src, dst) in enumerate(
            (
                (me_h, small.at[0]),
                (mr_h, small.at[1]),
                (go_h, go),
                (hid_h, hid),
                (ve_h, small.at[2]),
                (vr_h, small.at[3]),
                (acts_h, acts),
            )
        )
    ]
    for copy in loads:
        copy.start()

    barrier = pltpu.get_barrier_semaphore()
    peers = [me.zp(j) for j in range(1, NZ)] + [me.yp(j) for j in range(1, NY)]
    peers += [me.xp(j) for j in range(1, NX)] + [me.other()]
    for peer in peers:
        pl.semaphore_signal(barrier, inc=1, device_id=peer, device_id_type=MESH)

    loads[0].wait()
    loads[1].wait()
    we[me.z, me.y, me.kx] = small[0].astype(BF16)
    wr[me.z, me.y, me.kx] = small[1].astype(BF16)
    pl.semaphore_wait(barrier, len(peers))

    gather_e = Gather(net, me, we)
    gather_r = Gather(net, me, wr)
    gather_ne = Gather(net, me, ne)
    gather_nr = Gather(net, me, nr)
    scatter_e = Scatter(net, me, ge_refs)
    scatter_r = Scatter(net, me, gr_refs)
    norms_e = Norms(net, me, nz_e)
    norms_r = Norms(net, me, nz_r)
    tiles = channels // 256

    gather_e.along_z()
    loads[2].wait()
    loads[3].wait()

    def ge_tile(t, carry):
        cols = go[:, pl.ds(pl.multiple_of(t * 256, 256), 256)]
        value = lax.dot_general(
            cols, hid[...], (((0,), (0,)), ((), ())), preferred_element_type=F32
        )
        scatter_e.tile(t, value * inv_m)
        return carry

    lax.fori_loop(0, tiles, ge_tile, 0)
    scatter_e.cores()
    gather_e.middle()
    gather_r.along_z()
    gather_e.large()
    gather_r.middle()
    gather_e.forward()
    scatter_e.large()
    gather_e.finish()
    gather_e.arrived()

    def natural(w, t):
        block = w[t].reshape(NY * NK * NX, BLK, middle)
        return block.astype(F32).reshape(256, middle).astype(BF16)

    def flatten(t, carry):
        flat[pl.ds(pl.multiple_of(t * 256, 256), 256), :] = natural(we, t)
        return carry

    lax.fori_loop(0, tiles, flatten, 0)
    acc[...] = jnp.dot(go[...], flat[...], preferred_element_type=F32)
    gh[...] = jnp.where(hid[...].astype(F32) > 0, acc[...] * inv_m, 0.0).astype(BF16)
    loads[6].wait()

    def gr_tile(t, carry):
        cols = acts[:, pl.ds(pl.multiple_of(t * 256, 256), 256)]
        value = lax.dot_general(
            cols, gh[...], (((0,), (0,)), ((), ())), preferred_element_type=F32
        )
        scatter_r.tile(t, value * inv_c)
        return carry

    lax.fori_loop(0, tiles, gr_tile, 0)
    scatter_r.cores()
    scatter_e.forward()
    scatter_r.large()
    scatter_e.middle()
    scatter_r.forward()
    scatter_e.along_z()
    scatter_r.middle()
    gather_r.large()

    g_e = scatter_e.result()
    loads[4].wait()
    loads[5].wait()
    smallout[0] = g_e
    norms_e.start(0, stat_tile(small[0], g_e))
    scatter_r.along_z()
    tile_e = norms_e.finish(0)
    norms_e.start(1, tile_e)
    gather_r.forward()
    tile_e = norms_e.finish(1)
    norms_e.start(2, tile_e)
    g_r = scatter_r.result()
    norms_r.start(0, stat_tile(small[1], g_r))
    tile_e = norms_e.finish(2)
    norms_e.start(3, tile_e)
    tile_e = norms_e.finish(3)
    new_me, new_ve = updated(small[0], smallout[0], small[2], tile_e)
    ne[me.z, me.y, me.kx] = new_me.astype(BF16)
    gather_ne.along_z()
    smallout[0] = new_me
    smallout[1] = new_ve
    tile_r = norms_r.finish(0)
    norms_r.start(1, tile_r)
    gather_r.finish()
    tile_r = norms_r.finish(1)
    norms_r.start(2, tile_r)
    tile_r = norms_r.finish(2)
    norms_r.start(3, tile_r)
    tile_r = norms_r.finish(3)
    new_mr, new_vr = updated(small[1], g_r, small[3], tile_r)
    nr[me.z, me.y, me.kx] = new_mr.astype(BF16)
    gather_nr.along_z()
    smallout[2] = new_mr
    smallout[3] = new_vr
    gather_ne.middle()
    gather_ne.large()
    gather_nr.middle()
    gather_r.arrived()

    def gi_tile(t, carry):
        cols = pl.ds(pl.multiple_of(t * 256, 256), 256)
        back = lax.dot_general(
            gh[...], natural(wr, t), (((1,), (1,)), ((), ())), preferred_element_type=F32
        )
        gi[:, cols] = (go[:, cols].astype(F32) + back * inv_c).astype(BF16)
        return carry

    lax.fori_loop(0, tiles, gi_tile, 0)
    outs = [
        pltpu.make_async_copy(src, dst, out_sem.at[i])
        for i, (src, dst) in enumerate(
            (
                (gi, gi_h),
                (smallout.at[0], nme_h),
                (smallout.at[1], nve_h),
                (smallout.at[2], nmr_h),
                (smallout.at[3], nvr_h),
                (ne, we_h),
                (nr, wr_h),
            )
        )
    ]
    for copy in outs[:5]:
        copy.start()
    gather_ne.forward()
    gather_nr.large()
    gather_ne.finish()
    gather_nr.forward()
    gather_ne.arrived()
    outs[5].start()
    gather_nr.finish()
    gather_nr.arrived()
    outs[6].start()
    for unit in (
        gather_e, gather_r, gather_ne, gather_nr, scatter_e, scatter_r, norms_e, norms_r
    ):
        unit.drain()
    for copy in outs:
        copy.wait()
    assert net.used <= SEMS


def shards(acts, hid, go, mr, me_, vr, ve):
    rows, channels = acts.shape
    middle = hid.shape[1]
    half = middle // 2
    own = mr.shape
    whole = (NZ, NY, NK * NX, BLK, middle)
    scatter = (
        pltpu.VMEM((2, NK, 4, 32, BLK, half), BF16),
        pltpu.VMEM((2, 4, 32, BLK, half), BF16),
        pltpu.VMEM((2, 4, 32, BLK, half), BF16),
        pltpu.VMEM((2, 32, BLK, half), BF16),
        pltpu.VMEM((2, 32, BLK, half), BF16),
        pltpu.VMEM((2, 2, 32, BLK, half), BF16),
        pltpu.VMEM((2, 32, BLK, half), BF16),
        pltpu.VMEM((2, 3, NZ, BLK, half), BF16),
        pltpu.VMEM((NZ, BLK, middle), BF16),
        pltpu.VMEM((NZ - 1, BLK, middle), BF16),
    )
    norms = tuple(pltpu.VMEM((n, 8, 128), F32) for n in (NZ, NY, NX, NK))
    anyspace = pl.BlockSpec(memory_space=pl.ANY)
    out = pl.pallas_call(
        kernel,
        out_shape=(
            jax.ShapeDtypeStruct((rows, channels), BF16),
            jax.ShapeDtypeStruct(own, F32),
            jax.ShapeDtypeStruct(own, F32),
            jax.ShapeDtypeStruct(own, F32),
            jax.ShapeDtypeStruct(own, F32),
            jax.ShapeDtypeStruct(whole, BF16),
            jax.ShapeDtypeStruct(whole, BF16),
        ),
        in_specs=[anyspace] * 7,
        out_specs=(anyspace,) * 7,
        scratch_shapes=[
            pltpu.VMEM((rows, channels), BF16),
            pltpu.VMEM((rows, middle), BF16),
            pltpu.VMEM((rows, channels), BF16),
            pltpu.VMEM((4, *own), F32),
            pltpu.VMEM((4, *own), F32),
            pltpu.VMEM((rows, channels), BF16),
            pltpu.VMEM((rows, middle), BF16),
            pltpu.VMEM((rows, middle), F32),
            pltpu.VMEM(whole, BF16),
            pltpu.VMEM(whole, BF16),
            pltpu.VMEM(whole, BF16),
            pltpu.VMEM(whole, BF16),
            pltpu.VMEM((channels, middle), BF16),
            scatter,
            scatter,
            norms,
            norms,
            pltpu.SemaphoreType.DMA((SEMS,)),
            pltpu.SemaphoreType.DMA((SEMS,)),
            pltpu.SemaphoreType.DMA((7,)),
            pltpu.SemaphoreType.DMA((7,)),
        ],
        compiler_params=pltpu.CompilerParams(
            collective_id=0, has_side_effects=True, vmem_limit_bytes=60 * 1024 * 1024
        ),
    )(acts, hid, go, mr, me_, vr, ve)
    flat = (channels, middle)
    return (*out[:5], out[5].reshape(flat), out[6].reshape(flat))


def solution(mesh):
    split = P(ROWS_SPLIT, None)
    return jax.shard_map(
        shards,
        mesh=mesh,
        in_specs=(split,) * 7,
        out_specs=(split,) * 5 + (P(), P()),
        check_vma=False,
    )
```

```python
import jax
import jax.numpy as jnp
from jax import lax
from jax.experimental import pallas as pl
from jax.experimental.pallas import tpu as pltpu
from jax.sharding import PartitionSpec as P

MESH = pl.DeviceIdType.MESH
BF16 = jnp.bfloat16
F32 = jnp.float32
ROWS_SPLIT = ("gx", "gy", "gz")
NZ, NY, NX, NK = 8, 4, 4, 2
BLK = 8
FAR_FIRST = (4, 3, 5, 2, 6, 1, 7)
SEMS = 400
CHUNKS = 2


class Net:
    def __init__(self, send, recv):
        self.send, self.recv, self.used = send, recv, 0

    def put(self, src, dst, peer):
        at = self.used
        self.used += 1
        copy = pltpu.make_async_remote_copy(
            src_ref=src,
            dst_ref=dst,
            send_sem=self.send.at[at],
            recv_sem=self.recv.at[at],
            device_id=peer,
            device_id_type=MESH,
        )
        copy.start()
        return copy


class Place:
    def __init__(self):
        self.z = lax.axis_index("gx")
        gy = lax.axis_index("gy")
        self.y = gy // 2
        self.k = gy % 2
        self.x = lax.axis_index("gz")
        self.gy = gy
        self.kx = self.k * NX + self.x
        self.d = 1 - 2 * self.k

    def zp(self, j):
        return {"gx": (self.z + j) % NZ}

    def yp(self, j):
        return {"gy": ((self.y + j + NY) % NY) * 2 + self.k}

    def xp(self, j):
        return {"gz": (self.x + j + NX) % NX}

    def other(self):
        return {"gy": self.gy + 1 - 2 * self.k}


class Gather:
    def __init__(self, net, me, w):
        self.net, self.me, self.w = net, me, w
        half = w.shape[-1] // 2
        self.parts = (pl.ds(0, half), pl.ds(half, half))
        self.cores = []
        self.sent = []

    def put(self, ref, peer):
        copy = self.net.put(ref, ref, peer)
        self.sent.append(copy)
        return copy

    def along_z(self):
        me = self.me
        ref = self.w.at[me.z, me.y, me.kx]
        self.zs = [self.put(ref, me.zp(j)) for j in FAR_FIRST]

    def middle(self):
        me = self.me
        for copy in self.zs:
            copy.wait_recv()
        self.mids = []
        for part, peer in zip(self.parts, (me.yp, me.xp)):
            ref = self.w.at[:, me.y, me.kx, :, part]
            self.mids.append([self.put(ref, peer(j)) for j in (2, 1, 3)])

    def slab(self, part, off, chunk=None):
        me = self.me
        zs = slice(None)
        if chunk is not None:
            zs = pl.ds(chunk * (NZ // CHUNKS), NZ // CHUNKS)
        if part == 0:
            x = (me.x + off + NX) % NX
            return self.w.at[zs, :, me.k * NX + x, :, self.parts[0]]
        y = (me.y + off + NY) % NY
        return self.w.at[zs, y, pl.ds(me.k * NX, NX), :, self.parts[1]]

    def peer(self, part, off):
        return self.me.xp(off) if part == 0 else self.me.yp(off)

    def core(self, part, off, chunk=None):
        self.cores.append(self.put(self.slab(part, off, chunk), self.me.other()))

    def middle_arrived(self, part):
        for copy in self.mids[part]:
            copy.wait_recv()

    def large(self):
        d = self.me.d
        self.near = []
        for part in range(2):
            self.middle_arrived(part)
            ahead = [
                self.put(self.slab(part, 0, c), self.peer(part, d)) for c in range(CHUNKS)
            ]
            self.near.append((ahead, self.put(self.slab(part, 0), self.peer(part, -d))))
        for part in range(2):
            self.core(part, 0)

    def forward(self):
        d = self.me.d
        self.far = ([], [])
        for c in range(CHUNKS):
            for part in range(2):
                self.near[part][0][c].wait_recv()
                self.far[part].append(self.put(self.slab(part, -d, c), self.peer(part, d)))
        for part in range(2):
            self.core(part, -d)

    def finish(self):
        d = self.me.d
        for part in range(2):
            self.near[part][1].wait_recv()
            self.core(part, d)
        for c in range(CHUNKS):
            for part in range(2):
                self.far[part][c].wait_recv()
                self.core(part, 2, c)

    def arrived(self):
        for copy in self.cores:
            copy.wait_recv()

    def drain(self):
        for copy in self.sent:
            copy.wait_send()


class Strips:
    def __init__(self, net, me, zb, m):
        self.net, self.me, self.zb, self.m = net, me, zb, m
        self.sent = []

    def along_z(self, block):
        me = self.me
        self.zb[me.z] = block
        ref = self.zb.at[me.z]
        self.zs = [self.net.put(ref, ref, me.zp(j)) for j in FAR_FIRST]
        self.sent += self.zs

    def middle(self):
        me = self.me
        half = self.m.shape[-1]
        for copy in self.zs:
            copy.wait_recv()
        self.mids = []
        for part, peer, own in ((0, me.yp, me.y), (1, me.xp, me.x)):
            src = self.zb.at[:, :, pl.ds(part * half, half)]
            self.mids += [self.net.put(src, self.m.at[part, own], peer(j)) for j in (2, 1, 3)]
        self.sent += self.mids
        for part, own in ((0, me.y), (1, me.x)):
            self.m[part, own] = self.zb[:, :, pl.ds(part * half, half)]

    def arrived(self):
        for copy in self.mids:
            copy.wait_recv()

    def drain(self):
        for copy in self.sent:
            copy.wait_send()


def add_blocks(first, last, out, *terms):
    def step(i, carry):
        total = terms[0](i).astype(F32)
        for term in terms[1:]:
            total = total + term(i).astype(F32)
        out(i, total)
        return carry

    lax.fori_loop(first, last, step, 0)


class Scatter:
    def __init__(self, net, me, refs):
        self.net, self.me = net, me
        (self.p, self.c, self.s, self.f, self.t, self.r, self.a, self.m, self.b, self.q) = refs
        self.sent = []
        self.cs = ([], [])

    def put(self, src, dst, peer):
        copy = self.net.put(src, dst, peer)
        self.sent.append(copy)
        return copy

    def tile(self, t, value):
        half = value.shape[1] // 2
        for y in range(NY):
            for k in range(NK):
                for x in range(NX):
                    at = ((y * NK + k) * NX + x) * BLK
                    rows = value[at : at + BLK]
                    self.p[0, k, x, y, t] = rows[:, :half].astype(BF16)
                    self.p[1, k, y, x, t] = rows[:, half:].astype(BF16)

    def cores(self, first, count):
        me = self.me
        for part in range(2):
            zs = pl.ds(first, count)
            self.cs[part].append(
                self.put(
                    self.p.at[part, 1 - me.k, :, :, zs], self.c.at[part, :, :, zs], me.other()
                )
            )

    def peer(self, part, off):
        return self.me.xp(off) if part == 0 else self.me.yp(off)

    def index(self, part, off):
        return (self.me.x + off + NX) % NX if part == 0 else (self.me.y + off + NY) % NY

    def joined(self, part, off, first=0, count=4):
        me = self.me
        at = self.index(part, off)

        def out(i, total):
            self.s[part, at, i] = total.astype(BF16)

        add_blocks(
            first,
            first + count,
            out,
            lambda i: self.p[part, me.k, at, i],
            lambda i: self.c[part, at, i],
        )
        return self.s.at[part, at, pl.ds(first, count)]

    def large(self):
        d = self.me.d
        per = 4 // CHUNKS
        self.near = ([], [])
        for part in range(2):
            for copy in self.cs[part]:
                copy.wait_recv()
        for c in range(CHUNKS):
            for part in range(2):
                src = self.joined(part, 2, c * per, per)
                dst = self.f.at[part, pl.ds(c * per, per)]
                self.near[part].append(self.put(src, dst, self.peer(part, d)))
        self.side = [
            self.put(self.joined(part, -d), self.r.at[part, 0], self.peer(part, -d))
            for part in range(2)
        ]
        for part in range(2):
            self.joined(part, d)
            self.joined(part, 0)

    def forward(self):
        d = self.me.d
        per = 4 // CHUNKS
        self.far = ([], [])
        for c in range(CHUNKS):
            for part in range(2):
                self.near[part][c].wait_recv()
                at = self.index(part, d)

                def out(i, total, part=part):
                    self.t[part, i] = total.astype(BF16)

                add_blocks(
                    c * per,
                    (c + 1) * per,
                    out,
                    lambda i, part=part, at=at: self.s[part, at, i],
                    lambda i, part=part: self.f[part, i],
                )
                piece = pl.ds(c * per, per)
                self.far[part].append(
                    self.put(
                        self.t.at[part, piece], self.r.at[part, 1, piece], self.peer(part, d)
                    )
                )

    def middle(self):
        self.mids = []
        for part in range(2):
            self.side[part].wait_recv()
            for copy in self.far[part]:
                copy.wait_recv()
            at = self.index(part, 0)

            def out(i, total, part=part):
                self.a[part, i] = total.astype(BF16)

            add_blocks(
                0,
                4,
                out,
                lambda i, part=part, at=at: self.s[part, at, i],
                lambda i, part=part: self.r[part, 0, i],
                lambda i, part=part: self.r[part, 1, i],
            )
            copies = []
            for j in (2, 1, 3):
                to = self.index(1 - part, j)
                copies.append(
                    self.put(self.a.at[part, to], self.m.at[part, j - 1], self.peer(1 - part, j))
                )
            self.mids.append(copies)

    def along_z(self):
        me = self.me
        for part in range(2):
            for copy in self.mids[part]:
                copy.wait_recv()
            at = self.index(1 - part, 0)
            total = self.a[part, at].astype(F32)
            for j in range(3):
                total = total + self.m[part, j].astype(F32)
            half = total.shape[-1]
            self.b[:, :, pl.ds(part * half, half)] = total.astype(BF16)
        self.zs = []
        for j in FAR_FIRST:
            self.zs.append(self.put(self.b.at[(me.z + j) % NZ], self.q.at[j - 1], me.zp(j)))

    def result(self):
        for copy in self.zs:
            copy.wait_recv()
        total = self.b[self.me.z].astype(F32)
        for j in range(7):
            total = total + self.q[j].astype(F32)
        return total

    def drain(self):
        for copy in self.sent:
            copy.wait_send()


class Norms:
    def __init__(self, net, me, refs):
        self.net, self.me, self.refs = net, me, refs
        self.sent = []

    def start(self, axis, tile):
        me = self.me
        ref = self.refs[axis]
        own = (me.z, me.y, me.x, me.k)[axis]
        ref[own] = tile
        peers = (
            [me.zp(j) for j in FAR_FIRST],
            [me.yp(j) for j in (2, 1, 3)],
            [me.xp(j) for j in (2, 1, 3)],
            [me.other()],
        )[axis]
        self.flying = [self.net.put(ref.at[own], ref.at[own], peer) for peer in peers]
        self.sent += self.flying

    def finish(self, axis):
        ref = self.refs[axis]
        for copy in self.flying:
            copy.wait_recv()
        total = ref[0]
        for i in range(1, ref.shape[0]):
            total = total + ref[i]
        return total

    def drain(self):
        for copy in self.sent:
            copy.wait_send()


def fold(sq):
    lanes = sq[:, 0:128]
    for i in range(1, sq.shape[1] // 128):
        lanes = lanes + sq[:, 128 * i : 128 * (i + 1)]
    return jnp.sum(lanes, axis=0, keepdims=True)


def stat_tile(w, g):
    row = lax.broadcasted_iota(jnp.int32, (8, 128), 0)
    wrow = jnp.broadcast_to(fold(w * w), (8, 128))
    grow = jnp.broadcast_to(fold(g * g), (8, 128))
    return jnp.where(row == 0, wrow, jnp.where(row == 1, grow, 0.0))


def trust_of(tile):
    wsquare = jnp.sum(tile[0:1, :], axis=1, keepdims=True)
    gsquare = jnp.sum(tile[1:2, :], axis=1, keepdims=True)
    wnorm = jnp.sqrt(wsquare)
    gnorm = jnp.sqrt(gsquare)
    return wnorm / (gnorm + 5e-05 * wnorm)


def updated(master, grads, velocity, trust):
    new_velocity = 0.9 * velocity + trust * (grads + 5e-05 * master)
    new_master = master - 0.1 * new_velocity
    return new_master, new_velocity


def kernel(
    acts_h, hid_h, go_h, mr_h, me_h, vr_h, ve_h,
    gi, smallout, ne, nr,
    acts, hid, go, small, gh, acc,
    we, wr, flat, g_kept, az, am, gz, gm, ge_refs, gr_refs, nz_e, nz_r,
    send, recv, load,
):
    scope = jax.named_scope
    me = Place()
    net = Net(send, recv)
    channels = go.shape[1]
    middle = hid.shape[1]
    half = middle // 2
    inv_c = 1.0 / float(channels) ** 0.5
    inv_m = 1.0 / float(middle) ** 0.5

    loads = [
        pltpu.make_async_copy(src, dst, load.at[i])
        for i, (src, dst) in enumerate(
            (
                (me_h, small.at[0]),
                (mr_h, small.at[1]),
                (vr_h, small.at[3]),
                (ve_h, small.at[2]),
                (go_h, go),
                (hid_h, hid),
                (acts_h, acts),
            )
        )
    ]
    for copy in loads:
        copy.start()

    barrier = pltpu.get_barrier_semaphore()
    peers = [me.zp(j) for j in FAR_FIRST] + [me.yp(j) for j in (2, 1, 3)]
    peers += [me.xp(j) for j in (2, 1, 3)] + [me.other()]
    for peer in peers:
        pl.semaphore_signal(barrier, inc=1, device_id=peer, device_id_type=MESH)

    for copy in loads[:4]:
        copy.wait()
    we[me.z, me.y, me.kx] = small[0].astype(BF16)
    wr[me.z, me.y, me.kx] = small[1].astype(BF16)
    with scope("barrier"):
        pl.semaphore_wait(barrier, len(peers))

    gather_e = Gather(net, me, we)
    gather_r = Gather(net, me, wr)
    gather_ne = Gather(net, me, ne)
    gather_nr = Gather(net, me, nr)
    scatter_e = Scatter(net, me, ge_refs)
    scatter_r = Scatter(net, me, gr_refs)
    norms_e = Norms(net, me, nz_e)
    norms_r = Norms(net, me, nz_r)
    strips_a = Strips(net, me, az, am)
    strips_g = Strips(net, me, gz, gm)
    tiles = channels // 256

    def tile_cols(t):
        return pl.ds(pl.multiple_of(t * 256, 256), 256)

    def natural(w, t):
        block = w[t].reshape(NY * NK * NX, BLK, middle)
        return block.astype(F32).reshape(256, middle).astype(BF16)

    def ge_tile(t, carry):
        value = lax.dot_general(
            go[:, tile_cols(t)], hid[...], (((0,), (0,)), ((), ())), preferred_element_type=F32
        )
        scatter_e.tile(t, value * inv_m)
        return carry

    def gr_tile(t, carry):
        value = lax.dot_general(
            acts[:, tile_cols(t)], gh[...], (((0,), (0,)), ((), ())), preferred_element_type=F32
        )
        scatter_r.tile(t, value * inv_c)
        return carry

    def flatten(t, carry):
        flat[tile_cols(t), :] = natural(we, t)
        return carry

    def gi_tile(t, carry):
        cols = tile_cols(t)
        back = lax.dot_general(
            gh[...], natural(wr, t), (((1,), (1,)), ((), ())), preferred_element_type=F32
        )
        gi[:, cols] = (go[:, cols].astype(F32) + back * inv_c).astype(BF16)
        return carry

    def e_result():
        g = scatter_e.result()
        g_kept[0] = g
        norms_e.start(0, stat_tile(small[0], g))

    def r_result():
        g = scatter_r.result()
        g_kept[1] = g
        norms_r.start(0, stat_tile(small[1], g))
        strips_g.along_z((g + 5e-05 * small[1]).astype(BF16))

    def norm_step(norms, axis):
        norms.start(axis + 1, norms.finish(axis))

    def e_update():
        trust = trust_of(norms_e.finish(3))
        new_master, new_velocity = updated(small[0], g_kept[0], small[2], trust)
        ne[me.z, me.y, me.kx] = new_master.astype(BF16)
        gather_ne.along_z()
        smallout[0] = new_master
        smallout[1] = new_velocity

    def r_update():
        trust = trust_of(norms_r.finish(3))
        strips_g.arrived()
        step = jnp.broadcast_to(0.1 * trust, (BLK, half))

        def fill(i, carry):
            for z in range(NZ):
                for part in range(2):
                    block = am[part, i, z] - step * gm[part, i, z].astype(F32)
                    if part == 0:
                        nr[z, i, me.kx, :, pl.ds(0, half)] = block.astype(BF16)
                    else:
                        nr[z, me.y, me.k * NX + i, :, pl.ds(half, half)] = block.astype(BF16)
            return carry

        lax.fori_loop(0, 4, fill, 0)
        gather_nr.mids = ([], [])
        gather_nr.large()
        new_master, new_velocity = updated(small[1], g_kept[1], small[3], trust)
        smallout[2] = new_master
        smallout[3] = new_velocity

    def ge_part(first, count):
        lax.fori_loop(first, first + count, ge_tile, 0)
        scatter_e.cores(first, count)

    def gr_part(first, count):
        lax.fori_loop(first, first + count, gr_tile, 0)
        scatter_r.cores(first, count)

    def hidden():
        lax.fori_loop(0, tiles, flatten, 0)
        acc[...] = jnp.dot(go[...], flat[...], preferred_element_type=F32)
        gh[...] = jnp.where(hid[...].astype(F32) > 0, acc[...] * inv_m, 0.0).astype(BF16)

    program = [
        ("E z", gather_e.along_z),
        ("R z", gather_r.along_z),
        ("A z", lambda: strips_a.along_z(small[1] - 0.09 * small[3])),
        ("load go", loads[4].wait),
        ("load hid", loads[5].wait),
        ("GE tiles 0", lambda: ge_part(0, 4)),
        ("GE tiles 1", lambda: ge_part(4, 4)),
        ("E mid", gather_e.middle),
        ("GE large", scatter_e.large),
        ("E large", gather_e.large),
        ("R mid", gather_r.middle),
        ("E forward", gather_e.forward),
        ("GE forward", scatter_e.forward),
        ("E finish", gather_e.finish),
        ("A mid", strips_a.middle),
        ("E arrived", gather_e.arrived),
        ("hidden", hidden),
        ("GE mid", scatter_e.middle),
        ("load acts", loads[6].wait),
        ("GR tiles 0", lambda: gr_part(0, 4)),
        ("GR tiles 1", lambda: gr_part(4, 4)),
        ("GE z", scatter_e.along_z),
        ("GR large", scatter_r.large),
        ("GE result", e_result),
        ("GR forward", scatter_r.forward),
        ("norm e0", lambda: norm_step(norms_e, 0)),
        ("GR mid", scatter_r.middle),
        ("R large", gather_r.large),
        ("norm e1", lambda: norm_step(norms_e, 1)),
        ("GR z", scatter_r.along_z),
        ("norm e2", lambda: norm_step(norms_e, 2)),
        ("R forward", gather_r.forward),
        ("E update", e_update),
        ("GR result", r_result),
        ("R finish", gather_r.finish),
        ("NE mid", gather_ne.middle),
        ("A arrived", strips_a.arrived),
        ("norm r0", lambda: norm_step(norms_r, 0)),
        ("g mid", strips_g.middle),
        ("NE large", gather_ne.large),
        ("norm r1", lambda: norm_step(norms_r, 1)),
        ("NE forward", gather_ne.forward),
        ("norm r2", lambda: norm_step(norms_r, 2)),
        ("R update", r_update),
        ("R arrived", gather_r.arrived),
        ("gi", lambda: lax.fori_loop(0, tiles, gi_tile, 0)),
        ("NR forward", gather_nr.forward),
        ("NE finish", gather_ne.finish),
        ("NR finish", gather_nr.finish),
        ("NE arrived", gather_ne.arrived),
        ("NR arrived", gather_nr.arrived),
    ]
    for name, step in program:
        with scope(name.replace(" ", "_")):
            step()
    with scope("drain"):
        for unit in (
            gather_e, gather_r, gather_ne, gather_nr, scatter_e, scatter_r,
            norms_e, norms_r, strips_a, strips_g,
        ):
            unit.drain()
    assert net.used <= SEMS


def write_out(gi, small, ne, nr, gi_h, nmr_h, nme_h, nvr_h, nve_h, wr_h, we_h, sem):
    copies = [
        pltpu.make_async_copy(src, dst, sem.at[i])
        for i, (src, dst) in enumerate(
            (
                (gi, gi_h),
                (ne, we_h),
                (nr, wr_h),
                (small.at[0], nme_h),
                (small.at[1], nve_h),
                (small.at[2], nmr_h),
                (small.at[3], nvr_h),
            )
        )
    ]
    for copy in copies:
        copy.start()
    for copy in copies:
        copy.wait()


def shards(acts, hid, go, mr, me_, vr, ve):
    rows, channels = acts.shape
    middle = hid.shape[1]
    half = middle // 2
    own = mr.shape
    whole = (NZ, NY, NK * NX, BLK, middle)
    scatter = (
        pltpu.VMEM((2, NK, 4, 4, NZ, BLK, half), BF16),
        pltpu.VMEM((2, 4, 4, NZ, BLK, half), BF16),
        pltpu.VMEM((2, 4, 4, NZ, BLK, half), BF16),
        pltpu.VMEM((2, 4, NZ, BLK, half), BF16),
        pltpu.VMEM((2, 4, NZ, BLK, half), BF16),
        pltpu.VMEM((2, 2, 4, NZ, BLK, half), BF16),
        pltpu.VMEM((2, 4, NZ, BLK, half), BF16),
        pltpu.VMEM((2, 3, NZ, BLK, half), BF16),
        pltpu.VMEM((NZ, BLK, middle), BF16),
        pltpu.VMEM((NZ - 1, BLK, middle), BF16),
    )
    norms = tuple(pltpu.VMEM((n, 8, 128), F32) for n in (NZ, NY, NX, NK))
    in_hbm = pl.BlockSpec(memory_space=pltpu.HBM)
    vmem = pl.BlockSpec(memory_space=pltpu.VMEM)
    results = pl.pallas_call(
        kernel,
        out_shape=(
            pltpu.VMEM((rows, channels), BF16),
            pltpu.VMEM((4, *own), F32),
            pltpu.VMEM(whole, BF16),
            pltpu.VMEM(whole, BF16),
        ),
        in_specs=[in_hbm] * 7,
        out_specs=(vmem,) * 4,
        scratch_shapes=[
            pltpu.VMEM((rows, channels), BF16),
            pltpu.VMEM((rows, middle), BF16),
            pltpu.VMEM((rows, channels), BF16),
            pltpu.VMEM((4, *own), F32),
            pltpu.VMEM((rows, middle), BF16),
            pltpu.VMEM((rows, middle), F32),
            pltpu.VMEM(whole, BF16),
            pltpu.VMEM(whole, BF16),
            pltpu.VMEM((channels, middle), BF16),
            pltpu.VMEM((2, *own), F32),
            pltpu.VMEM((NZ, BLK, middle), F32),
            pltpu.VMEM((2, 4, NZ, BLK, half), F32),
            pltpu.VMEM((NZ, BLK, middle), BF16),
            pltpu.VMEM((2, 4, NZ, BLK, half), BF16),
            scatter,
            scatter,
            norms,
            norms,
            pltpu.SemaphoreType.DMA((SEMS,)),
            pltpu.SemaphoreType.DMA((SEMS,)),
            pltpu.SemaphoreType.DMA((7,)),
        ],
        compiler_params=pltpu.CompilerParams(
            collective_id=0, has_side_effects=True, vmem_limit_bytes=44 * 1024 * 1024
        ),
    )(acts, hid, go, mr, me_, vr, ve)
    out = pl.pallas_call(
        write_out,
        out_shape=(
            jax.ShapeDtypeStruct((rows, channels), BF16),
            jax.ShapeDtypeStruct(own, F32),
            jax.ShapeDtypeStruct(own, F32),
            jax.ShapeDtypeStruct(own, F32),
            jax.ShapeDtypeStruct(own, F32),
            jax.ShapeDtypeStruct(whole, BF16),
            jax.ShapeDtypeStruct(whole, BF16),
        ),
        in_specs=[vmem] * 4,
        out_specs=(in_hbm,) * 7,
        scratch_shapes=[pltpu.SemaphoreType.DMA((7,))],
        compiler_params=pltpu.CompilerParams(vmem_limit_bytes=4 * 1024 * 1024),
    )(*results)
    flat = (channels, middle)
    return (*out[:5], out[5].reshape(flat), out[6].reshape(flat))


def solution(mesh):
    split = P(ROWS_SPLIT, None)
    return jax.shard_map(
        shards,
        mesh=mesh,
        in_specs=(split,) * 7,
        out_specs=(split,) * 5 + (P(), P()),
        check_vma=False,
    )
```

```python
import jax
import jax.numpy as jnp
from jax import lax
from jax.experimental import pallas as pl
from jax.experimental.pallas import tpu as pltpu
from jax.sharding import PartitionSpec as P

MESH = pl.DeviceIdType.MESH
BF16 = jnp.bfloat16
F32 = jnp.float32
ROWS_SPLIT = ("gx", "gy", "gz")
NZ, NY, NX, NK = 8, 4, 4, 2
BLK = 8
FAR_FIRST = (4, 3, 5, 2, 6, 1, 7)
STRIPS = (2, 1, 3, 0)
SENDS = 10
RECVS = 137
MID_ORDER = (1, 3, 2)


class Group:
    def __init__(self, net, sem):
        self.net, self.sem, self.bytes = net, sem, 0

    def wait(self):
        self.net.wait(self.sem, self.bytes)


class Net:
    def __init__(self, send, recv, spare):
        self.send, self.recv, self.spare = send, recv, spare
        self.used = self.units = 0

    def unit(self):
        self.units += 1
        return Group(self, self.send.at[self.units - 1])

    def group(self):
        self.used += 1
        return Group(self, self.recv.at[self.used - 1])

    def put(self, src, dst, peer, unit, group):
        size = src.dtype.itemsize
        for extent in src.shape:
            size *= extent
        unit.bytes += size
        group.bytes += size
        pltpu.make_async_remote_copy(
            src_ref=src,
            dst_ref=dst,
            send_sem=unit.sem,
            recv_sem=group.sem,
            device_id=peer,
            device_id_type=MESH,
        ).start()

    def wait(self, sem, size):
        blocks, rest = divmod(size, 4096)
        assert rest == 0
        ref = self.spare.at[pl.ds(0, blocks)]
        pltpu.make_async_copy(ref, ref, sem).wait()


class Place:
    def __init__(self):
        self.z = lax.axis_index("gx")
        gy = lax.axis_index("gy")
        self.y = gy // 2
        self.k = gy % 2
        self.x = lax.axis_index("gz")
        self.gy = gy
        self.kx = self.k * NX + self.x
        self.d = 1 - 2 * self.k

    def zp(self, j):
        return {"gx": (self.z + j) % NZ}

    def yp(self, j):
        return {"gy": ((self.y + j + NY) % NY) * 2 + self.k}

    def xp(self, j):
        return {"gz": (self.x + j + NX) % NX}

    def other(self):
        return {"gy": self.gy + 1 - 2 * self.k}


class Gather:
    def __init__(self, net, me, w):
        self.net, self.me, self.w = net, me, w
        half = w.shape[-1] // 2
        self.parts = (pl.ds(0, half), pl.ds(half, half))
        self.unit = net.unit()
        self.cores = net.group()
        self.ahead = ({}, {})
        self.side = [net.group() for part in range(2)]
        self.far = [[net.group(), net.group()] for part in range(2)]

    def put(self, ref, peer, group):
        self.net.put(ref, ref, peer, self.unit, group)

    def along_z(self):
        me = self.me
        ref = self.w.at[me.z, me.y, me.kx]
        self.zs = self.net.group()
        for j in FAR_FIRST:
            self.put(ref, me.zp(j), self.zs)

    def at(self, part, large, mid):
        me = self.me
        x = (me.x + (large if part == 0 else mid) + NX) % NX
        y = (me.y + (mid if part == 0 else large) + NY) % NY
        return self.w.at[:, y, me.k * NX + x, :, self.parts[part]]

    def slab(self, part, off):
        me = self.me
        if part == 0:
            x = (me.x + off + NX) % NX
            return self.w.at[:, :, me.k * NX + x, :, self.parts[0]]
        y = (me.y + off + NY) % NY
        return self.w.at[:, y, pl.ds(me.k * NX, NX), :, self.parts[1]]

    def peer(self, part, off):
        return self.me.xp(off) if part == 0 else self.me.yp(off)

    def core(self, ref):
        self.put(ref, self.me.other(), self.cores)

    def near(self, part, mid):
        d = self.me.d
        self.ahead[part][mid] = self.net.group()
        self.put(self.at(part, 0, mid), self.peer(part, d), self.ahead[part][mid])
        self.put(self.at(part, 0, mid), self.peer(part, -d), self.side[part])

    def middle(self):
        self.zs.wait()
        self.mids = [{j: self.net.group() for j in MID_ORDER} for part in range(2)]
        for j in MID_ORDER:
            for part in range(2):
                self.put(self.at(part, 0, 0), self.peer(1 - part, j), self.mids[part][j])
        for part in range(2):
            self.near(part, 0)

    def near_one(self):
        for j in (1, 3):
            for part in range(2):
                self.mids[part][j].wait()
                self.near(part, -j)

    def near_two(self):
        for part in range(2):
            self.mids[part][2].wait()
            self.near(part, -2)
        for part in range(2):
            self.core(self.slab(part, 0))

    def near_all(self):
        for mid in (0, -1, -3, -2):
            for part in range(2):
                self.near(part, mid)
        for part in range(2):
            self.core(self.slab(part, 0))

    def forward(self, *mids):
        d = self.me.d
        for mid in mids:
            for part in range(2):
                self.ahead[part][mid].wait()
                group = self.far[part][0 if mid in (0, -1) else 1]
                self.put(self.at(part, -d, mid), self.peer(part, d), group)
        if -2 in mids:
            for part in range(2):
                self.core(self.slab(part, -d))

    def finish(self):
        d = self.me.d
        for part in range(2):
            self.side[part].wait()
            self.core(self.slab(part, d))
        for i, mids in enumerate(((0, -1), (-3, -2))):
            for part in range(2):
                self.far[part][i].wait()
                for mid in mids:
                    self.core(self.at(part, 2, mid))

    def arrived(self):
        self.cores.wait()


class Strips:
    def __init__(self, net, me, zb, m):
        self.net, self.me, self.zb, self.m = net, me, zb, m
        self.unit, self.zs, self.mids = net.unit(), net.group(), net.group()

    def along_z(self, block):
        me = self.me
        self.zb[me.z] = block
        ref = self.zb.at[me.z]
        for j in FAR_FIRST:
            self.net.put(ref, ref, me.zp(j), self.unit, self.zs)

    def middle(self):
        me = self.me
        half = self.m.shape[-1]
        self.zs.wait()
        for j in (2, 1, 3):
            for part, peer, own in ((0, me.yp, me.y), (1, me.xp, me.x)):
                src = self.zb.at[:, :, pl.ds(part * half, half)]
                self.net.put(src, self.m.at[part, own], peer(j), self.unit, self.mids)
        for part, own in ((0, me.y), (1, me.x)):
            self.m[part, own] = self.zb[:, :, pl.ds(part * half, half)]

    def arrived(self):
        self.mids.wait()


class Scatter:
    def __init__(self, net, me, refs):
        self.net, self.me = net, me
        (self.p, self.c, self.s, self.f, self.t, self.r, self.a, self.m, self.b, self.q) = refs
        self.unit = net.unit()
        self.cs = net.group()
        self.near = [[net.group() for mid in range(4)] for part in range(2)]
        self.far = [[net.group() for mid in range(4)] for part in range(2)]
        self.side = [net.group() for part in range(2)]
        self.mids = [net.group() for part in range(2)]
        self.zs = net.group()

    def put(self, src, dst, peer, group):
        self.net.put(src, dst, peer, self.unit, group)

    def tile(self, t, value):
        half = value.shape[1] // 2
        for y in range(NY):
            for k in range(NK):
                for x in range(NX):
                    at = ((y * NK + k) * NX + x) * BLK
                    rows = value[at : at + BLK]
                    self.p[0, k, x, y, t] = rows[:, :half].astype(BF16)
                    self.p[1, k, y, x, t] = rows[:, half:].astype(BF16)

    def cores(self, first, count):
        me = self.me
        zs = pl.ds(first, count)
        for part in range(2):
            self.put(
                self.p.at[part, 1 - me.k, :, :, zs],
                self.c.at[part, :, :, zs],
                me.other(),
                self.cs,
            )

    def peer(self, part, off):
        return self.me.xp(off) if part == 0 else self.me.yp(off)

    def index(self, part, off):
        return (self.me.x + off + NX) % NX if part == 0 else (self.me.y + off + NY) % NY

    def joined(self, part, off, mid):
        at, i = self.index(part, off), self.index(1 - part, mid)
        total = self.p[part, self.me.k, at, i].astype(F32) + self.c[part, at, i].astype(F32)
        self.s[part, at, i] = total.astype(BF16)
        return self.s.at[part, at, i]

    def large(self):
        d = self.me.d
        self.cs.wait()
        for mid in STRIPS:
            for part in range(2):
                dst = self.f.at[part, self.index(1 - part, mid)]
                src = self.joined(part, 2, mid)
                self.put(src, dst, self.peer(part, d), self.near[part][mid])
        for mid in STRIPS:
            for part in range(2):
                dst = self.r.at[part, 0, self.index(1 - part, mid)]
                src = self.joined(part, -d, mid)
                self.put(src, dst, self.peer(part, -d), self.side[part])
        for mid in STRIPS:
            for part in range(2):
                self.joined(part, d, mid)
                self.joined(part, 0, mid)

    def forward(self):
        d = self.me.d
        for mid in STRIPS:
            for part in range(2):
                self.near[part][mid].wait()
                i = self.index(1 - part, mid)
                total = self.s[part, self.index(part, d), i].astype(F32)
                total = total + self.f[part, i].astype(F32)
                self.t[part, i] = total.astype(BF16)
                dst = self.r.at[part, 1, i]
                self.put(self.t.at[part, i], dst, self.peer(part, d), self.far[part][mid])

    def middle(self):
        for part in range(2):
            self.side[part].wait()
        for mid in STRIPS:
            for part in range(2):
                self.far[part][mid].wait()
                i = self.index(1 - part, mid)
                total = self.s[part, self.index(part, 0), i].astype(F32)
                total = total + self.r[part, 0, i].astype(F32)
                total = total + self.r[part, 1, i].astype(F32)
                self.a[part, i] = total.astype(BF16)
                if mid:
                    dst = self.m.at[part, mid - 1]
                    self.put(self.a.at[part, i], dst, self.peer(1 - part, mid), self.mids[part])

    def along_z(self):
        me = self.me
        for part in range(2):
            self.mids[part].wait()
            at = self.index(1 - part, 0)
            total = self.a[part, at].astype(F32)
            for j in range(3):
                total = total + self.m[part, j].astype(F32)
            half = total.shape[-1]
            self.b[:, :, pl.ds(part * half, half)] = total.astype(BF16)
        for j in FAR_FIRST:
            self.put(self.b.at[(me.z + j) % NZ], self.q.at[j - 1], me.zp(j), self.zs)

    def result(self):
        self.zs.wait()
        total = self.b[self.me.z].astype(F32)
        for j in range(7):
            total = total + self.q[j].astype(F32)
        return total


class Norms:
    def __init__(self, net, me, refs):
        self.net, self.me, self.refs = net, me, refs
        self.unit = net.unit()
        self.groups = [net.group() for axis in range(4)]

    def start(self, axis, tile):
        me = self.me
        ref = self.refs[axis]
        own = (me.z, me.y, me.x, me.k)[axis]
        ref[own] = tile
        peers = (
            [me.zp(j) for j in FAR_FIRST],
            [me.yp(j) for j in (2, 1, 3)],
            [me.xp(j) for j in (2, 1, 3)],
            [me.other()],
        )[axis]
        for peer in peers:
            self.net.put(ref.at[own], ref.at[own], peer, self.unit, self.groups[axis])

    def finish(self, axis):
        ref = self.refs[axis]
        self.groups[axis].wait()
        total = ref[0]
        for i in range(1, ref.shape[0]):
            total = total + ref[i]
        return total


def fold(sq):
    lanes = sq[:, 0:128]
    for i in range(1, sq.shape[1] // 128):
        lanes = lanes + sq[:, 128 * i : 128 * (i + 1)]
    return jnp.sum(lanes, axis=0, keepdims=True)


def stat_tile(w, g):
    row = lax.broadcasted_iota(jnp.int32, (8, 128), 0)
    wrow = jnp.broadcast_to(fold(w * w), (8, 128))
    grow = jnp.broadcast_to(fold(g * g), (8, 128))
    return jnp.where(row == 0, wrow, jnp.where(row == 1, grow, 0.0))


def trust_of(tile):
    wsquare = jnp.sum(tile[0:1, :], axis=1, keepdims=True)
    gsquare = jnp.sum(tile[1:2, :], axis=1, keepdims=True)
    wnorm = jnp.sqrt(wsquare)
    gnorm = jnp.sqrt(gsquare)
    return wnorm / (gnorm + 5e-05 * wnorm)


def updated(master, grads, velocity, trust):
    new_velocity = 0.9 * velocity + trust * (grads + 5e-05 * master)
    new_master = master - 0.1 * new_velocity
    return new_master, new_velocity


def kernel(
    acts_h, hid_h, go_h, mr_h, me_h, vr_h, ve_h,
    gi, smallout, ne, nr,
    acts, hid, go, small, gh, acc,
    we, wr, flat, g_kept, az, am, gz, gm, ge_refs, gr_refs, nz_e, nz_r,
    send, recv, load, spare,
):
    scope = jax.named_scope
    me = Place()
    net = Net(send, recv, spare)
    channels = go.shape[1]
    middle = hid.shape[1]
    half = middle // 2
    inv_c = 1.0 / float(channels) ** 0.5
    inv_m = 1.0 / float(middle) ** 0.5

    loads = [
        pltpu.make_async_copy(src, dst, load.at[i])
        for i, (src, dst) in enumerate(
            (
                (me_h, small.at[0]),
                (mr_h, small.at[1]),
                (vr_h, small.at[3]),
                (ve_h, small.at[2]),
                (go_h, go),
                (hid_h, hid),
                (acts_h, acts),
            )
        )
    ]
    for copy in loads:
        copy.start()

    barrier = pltpu.get_barrier_semaphore()
    peers = [me.zp(j) for j in FAR_FIRST] + [me.yp(j) for j in (2, 1, 3)]
    peers += [me.xp(j) for j in (2, 1, 3)] + [me.other()]
    for peer in peers:
        pl.semaphore_signal(barrier, inc=1, device_id=peer, device_id_type=MESH)

    for copy in loads[:4]:
        copy.wait()
    we[me.z, me.y, me.kx] = small[0].astype(BF16)
    wr[me.z, me.y, me.kx] = small[1].astype(BF16)
    with scope("barrier"):
        pl.semaphore_wait(barrier, len(peers))

    gather_e = Gather(net, me, we)
    gather_r = Gather(net, me, wr)
    gather_ne = Gather(net, me, ne)
    gather_nr = Gather(net, me, nr)
    scatter_e = Scatter(net, me, ge_refs)
    scatter_r = Scatter(net, me, gr_refs)
    norms_e = Norms(net, me, nz_e)
    norms_r = Norms(net, me, nz_r)
    strips_a = Strips(net, me, az, am)
    strips_g = Strips(net, me, gz, gm)
    tiles = channels // 256

    def tile_cols(t):
        return pl.ds(pl.multiple_of(t * 256, 256), 256)

    def natural(w, t):
        block = w[t].reshape(NY * NK * NX, BLK, middle)
        return block.astype(F32).reshape(256, middle).astype(BF16)

    def ge_tile(t, carry):
        value = lax.dot_general(
            go[:, tile_cols(t)], hid[...], (((0,), (0,)), ((), ())), preferred_element_type=F32
        )
        scatter_e.tile(t, value * inv_m)
        return carry

    def gr_tile(t, carry):
        value = lax.dot_general(
            acts[:, tile_cols(t)], gh[...], (((0,), (0,)), ((), ())), preferred_element_type=F32
        )
        scatter_r.tile(t, value * inv_c)
        return carry

    def flatten(t, carry):
        flat[tile_cols(t), :] = natural(we, t)
        return carry

    def gi_tile(t, carry):
        cols = tile_cols(t)
        back = lax.dot_general(
            gh[...], natural(wr, t), (((1,), (1,)), ((), ())), preferred_element_type=F32
        )
        gi[:, cols] = (go[:, cols].astype(F32) + back * inv_c).astype(BF16)
        return carry

    def e_result():
        g = scatter_e.result()
        g_kept[0] = g
        norms_e.start(0, stat_tile(small[0], g))

    def r_result():
        g = scatter_r.result()
        g_kept[1] = g
        norms_r.start(0, stat_tile(small[1], g))
        strips_g.along_z((g + 5e-05 * small[1]).astype(BF16))

    def norm_step(norms, axis):
        norms.start(axis + 1, norms.finish(axis))

    def e_update():
        trust = trust_of(norms_e.finish(3))
        new_master, new_velocity = updated(small[0], g_kept[0], small[2], trust)
        ne[me.z, me.y, me.kx] = new_master.astype(BF16)
        gather_ne.along_z()
        smallout[0] = new_master
        smallout[1] = new_velocity

    def r_update():
        trust = trust_of(norms_r.finish(3))
        strips_g.arrived()
        step = jnp.broadcast_to(0.1 * trust, (BLK, half))

        def fill(i, carry):
            for z in range(NZ):
                for part in range(2):
                    block = am[part, i, z] - step * gm[part, i, z].astype(F32)
                    if part == 0:
                        nr[z, i, me.kx, :, pl.ds(0, half)] = block.astype(BF16)
                    else:
                        nr[z, me.y, me.k * NX + i, :, pl.ds(half, half)] = block.astype(BF16)
            return carry

        lax.fori_loop(0, 4, fill, 0)
        gather_nr.near_all()
        new_master, new_velocity = updated(small[1], g_kept[1], small[3], trust)
        smallout[2] = new_master
        smallout[3] = new_velocity

    def ge_part(first, count):
        lax.fori_loop(first, first + count, ge_tile, 0)
        scatter_e.cores(first, count)

    def gr_part(first, count):
        lax.fori_loop(first, first + count, gr_tile, 0)
        scatter_r.cores(first, count)

    def hidden():
        lax.fori_loop(0, tiles, flatten, 0)
        acc[...] = jnp.dot(go[...], flat[...], preferred_element_type=F32)
        gh[...] = jnp.where(hid[...].astype(F32) > 0, acc[...] * inv_m, 0.0).astype(BF16)

    program = [
        ("E z", gather_e.along_z),
        ("R z", gather_r.along_z),
        ("A z", lambda: strips_a.along_z(small[1] - 0.09 * small[3])),
        ("load go", loads[4].wait),
        ("load hid", loads[5].wait),
        ("GE tiles 0", lambda: ge_part(0, 4)),
        ("GE tiles 1", lambda: ge_part(4, 4)),
        ("E mid", gather_e.middle),
        ("GE large", scatter_e.large),
        ("E near 1", gather_e.near_one),
        ("E fwd 0", lambda: gather_e.forward(0)),
        ("E near 2", gather_e.near_two),
        ("E fwd 1", lambda: gather_e.forward(-1, -3)),
        ("E fwd 2", lambda: gather_e.forward(-2)),
        ("GE forward", scatter_e.forward),
        ("R mid", gather_r.middle),
        ("E finish", gather_e.finish),
        ("R near 1", gather_r.near_one),
        ("R near 2", gather_r.near_two),
        ("E arrived", gather_e.arrived),
        ("GE mid", scatter_e.middle),
        ("hidden", hidden),
        ("load acts", loads[6].wait),
        ("GR tiles 0", lambda: gr_part(0, 4)),
        ("R fwd", lambda: gather_r.forward(0, -1, -3, -2)),
        ("GR tiles 1", lambda: gr_part(4, 4)),
        ("GE z", scatter_e.along_z),
        ("A mid", strips_a.middle),
        ("GR large", scatter_r.large),
        ("GR forward", scatter_r.forward),
        ("GE result", e_result),
        ("GR mid", scatter_r.middle),
        ("norm e0", lambda: norm_step(norms_e, 0)),
        ("R finish", gather_r.finish),
        ("GR z", scatter_r.along_z),
        ("norm e1", lambda: norm_step(norms_e, 1)),
        ("norm e2", lambda: norm_step(norms_e, 2)),
        ("GR result", r_result),
        ("E update", e_update),
        ("A arrived", strips_a.arrived),
        ("norm r0", lambda: norm_step(norms_r, 0)),
        ("g mid", strips_g.middle),
        ("norm r1", lambda: norm_step(norms_r, 1)),
        ("NE mid", gather_ne.middle),
        ("norm r2", lambda: norm_step(norms_r, 2)),
        ("NE near 1", gather_ne.near_one),
        ("R update", r_update),
        ("NE fwd 0", lambda: gather_ne.forward(0)),
        ("NE near 2", gather_ne.near_two),
        ("R arrived", gather_r.arrived),
        ("gi", lambda: lax.fori_loop(0, tiles, gi_tile, 0)),
        ("NR fwd", lambda: gather_nr.forward(0, -1, -3, -2)),
        ("NE fwd 1", lambda: gather_ne.forward(-1, -3, -2)),
        ("NR finish", gather_nr.finish),
        ("NE finish", gather_ne.finish),
        ("NR arrived", gather_nr.arrived),
        ("NE arrived", gather_ne.arrived),
    ]
    for name, step in program:
        with scope(name.replace(" ", "_")):
            step()
    with scope("drain"):
        for unit in (
            gather_e, gather_r, gather_ne, gather_nr, scatter_e, scatter_r,
            norms_e, norms_r, strips_a, strips_g,
        ):
            unit.unit.wait()
    assert (net.units, net.used) == (SENDS, RECVS)


def write_out(gi, small, ne, nr, gi_h, nmr_h, nme_h, nvr_h, nve_h, wr_h, we_h, sem):
    copies = [
        pltpu.make_async_copy(src, dst, sem.at[i])
        for i, (src, dst) in enumerate(
            (
                (gi, gi_h),
                (ne, we_h),
                (nr, wr_h),
                (small.at[0], nme_h),
                (small.at[1], nve_h),
                (small.at[2], nmr_h),
                (small.at[3], nvr_h),
            )
        )
    ]
    for copy in copies:
        copy.start()
    for copy in copies:
        copy.wait()


def shards(acts, hid, go, mr, me_, vr, ve):
    rows, channels = acts.shape
    middle = hid.shape[1]
    half = middle // 2
    own = mr.shape
    whole = (NZ, NY, NK * NX, BLK, middle)
    scatter = (
        pltpu.VMEM((2, NK, 4, 4, NZ, BLK, half), BF16),
        pltpu.VMEM((2, 4, 4, NZ, BLK, half), BF16),
        pltpu.VMEM((2, 4, 4, NZ, BLK, half), BF16),
        pltpu.VMEM((2, 4, NZ, BLK, half), BF16),
        pltpu.VMEM((2, 4, NZ, BLK, half), BF16),
        pltpu.VMEM((2, 2, 4, NZ, BLK, half), BF16),
        pltpu.VMEM((2, 4, NZ, BLK, half), BF16),
        pltpu.VMEM((2, 3, NZ, BLK, half), BF16),
        pltpu.VMEM((NZ, BLK, middle), BF16),
        pltpu.VMEM((NZ - 1, BLK, middle), BF16),
    )
    norms = tuple(pltpu.VMEM((n, 8, 128), F32) for n in (NZ, NY, NX, NK))
    in_hbm = pl.BlockSpec(memory_space=pltpu.HBM)
    vmem = pl.BlockSpec(memory_space=pltpu.VMEM)
    args = [pltpu.with_memory_space_constraint(a, pltpu.HBM) for a in (acts, hid, go, mr, me_, vr, ve)]
    results = pl.pallas_call(
        kernel,
        out_shape=(
            pltpu.VMEM((rows, channels), BF16),
            pltpu.VMEM((4, *own), F32),
            pltpu.VMEM(whole, BF16),
            pltpu.VMEM(whole, BF16),
        ),
        in_specs=[in_hbm] * 7,
        out_specs=(vmem,) * 4,
        scratch_shapes=[
            pltpu.VMEM((rows, channels), BF16),
            pltpu.VMEM((rows, middle), BF16),
            pltpu.VMEM((rows, channels), BF16),
            pltpu.VMEM((4, *own), F32),
            pltpu.VMEM((rows, middle), BF16),
            pltpu.VMEM((rows, middle), F32),
            pltpu.VMEM(whole, BF16),
            pltpu.VMEM(whole, BF16),
            pltpu.VMEM((channels, middle), BF16),
            pltpu.VMEM((2, *own), F32),
            pltpu.VMEM((NZ, BLK, middle), F32),
            pltpu.VMEM((2, 4, NZ, BLK, half), F32),
            pltpu.VMEM((NZ, BLK, middle), BF16),
            pltpu.VMEM((2, 4, NZ, BLK, half), BF16),
            scatter,
            scatter,
            norms,
            norms,
            pltpu.SemaphoreType.DMA((SENDS,)),
            pltpu.SemaphoreType.DMA((RECVS,)),
            pltpu.SemaphoreType.DMA((7,)),
            pltpu.VMEM((512, BLK, half), BF16),
        ],
        compiler_params=pltpu.CompilerParams(
            collective_id=0, has_side_effects=True, vmem_limit_bytes=44 * 1024 * 1024
        ),
    )(*args)
    out = pl.pallas_call(
        write_out,
        out_shape=(
            jax.ShapeDtypeStruct((rows, channels), BF16),
            jax.ShapeDtypeStruct(own, F32),
            jax.ShapeDtypeStruct(own, F32),
            jax.ShapeDtypeStruct(own, F32),
            jax.ShapeDtypeStruct(own, F32),
            jax.ShapeDtypeStruct(whole, BF16),
            jax.ShapeDtypeStruct(whole, BF16),
        ),
        in_specs=[vmem] * 4,
        out_specs=(in_hbm,) * 7,
        scratch_shapes=[pltpu.SemaphoreType.DMA((7,))],
        compiler_params=pltpu.CompilerParams(vmem_limit_bytes=4 * 1024 * 1024),
    )(*results)
    flat = (channels, middle)
    return (*out[:5], out[5].reshape(flat), out[6].reshape(flat))


def solution(mesh):
    split = P(ROWS_SPLIT, None)
    return jax.shard_map(
        shards,
        mesh=mesh,
        in_specs=(split,) * 7,
        out_specs=(split,) * 5 + (P(), P()),
        check_vma=False,
    )
```

```python
import jax
import jax.numpy as jnp
from jax import lax
from jax.experimental import pallas as pl
from jax.experimental.pallas import tpu as pltpu
from jax.sharding import PartitionSpec as P

MESH = pl.DeviceIdType.MESH
BF16 = jnp.bfloat16
F32 = jnp.float32
ROWS_SPLIT = ("gx", "gy", "gz")
NZ, NY, NX, NK = 8, 4, 4, 2
BLK = 8
FAR_FIRST = (4, 3, 5, 2, 6, 1, 7)
STRIPS = (2, 1, 3, 0)
PLANE = [(jy, jx) for jy in (2, 1, 3, 0) for jx in (2, 1, 3, 0)][:-1]
SENDS = 10
RECVS = 120
MID_ORDER = (1, 3, 2)


class Group:
    def __init__(self, net, sem):
        self.net, self.sem, self.bytes = net, sem, 0

    def wait(self):
        self.net.wait(self.sem, self.bytes)


class Net:
    def __init__(self, send, recv, spare):
        self.send, self.recv, self.spare = send, recv, spare
        self.used = self.units = 0

    def unit(self):
        self.units += 1
        return Group(self, self.send.at[self.units - 1])

    def group(self):
        self.used += 1
        return Group(self, self.recv.at[self.used - 1])

    def put(self, src, dst, peer, unit, group):
        size = src.dtype.itemsize
        for extent in src.shape:
            size *= extent
        unit.bytes += size
        group.bytes += size
        pltpu.make_async_remote_copy(
            src_ref=src,
            dst_ref=dst,
            send_sem=unit.sem,
            recv_sem=group.sem,
            device_id=peer,
            device_id_type=MESH,
        ).start()

    def wait(self, sem, size):
        blocks, rest = divmod(size, 4096)
        assert rest == 0
        ref = self.spare.at[pl.ds(0, blocks)]
        pltpu.make_async_copy(ref, ref, sem).wait()


class Place:
    def __init__(self):
        self.z = lax.axis_index("gx")
        gy = lax.axis_index("gy")
        self.y = gy // 2
        self.k = gy % 2
        self.x = lax.axis_index("gz")
        self.gy = gy
        self.kx = self.k * NX + self.x
        self.d = 1 - 2 * self.k

    def zp(self, j):
        return {"gx": (self.z + j + NZ) % NZ}

    def plane(self, jy, jk, jx):
        y = (self.y + jy) % NY
        return {"gy": y * NK + (self.k + jk) % NK, "gz": (self.x + jx) % NX}

    def yp(self, j):
        return {"gy": ((self.y + j + NY) % NY) * 2 + self.k}

    def xp(self, j):
        return {"gz": (self.x + j + NX) % NX}

    def other(self):
        return {"gy": self.gy + 1 - 2 * self.k}


class Gather:
    def __init__(self, net, me, w):
        self.net, self.me, self.w = net, me, w
        half = w.shape[-1] // 2
        self.parts = (pl.ds(0, half), pl.ds(half, half))
        self.unit = net.unit()
        self.cores = net.group()
        self.ahead = ({}, {})
        self.side = [net.group() for part in range(2)]
        self.far = [[net.group(), net.group()] for part in range(2)]

    def put(self, ref, peer, group):
        self.net.put(ref, ref, peer, self.unit, group)

    def along_z(self):
        me = self.me
        ref = self.w.at[me.z, me.y, me.kx]
        self.zs = self.net.group()
        for j in FAR_FIRST:
            self.put(ref, me.zp(j), self.zs)

    def at(self, part, large, mid):
        me = self.me
        x = (me.x + (large if part == 0 else mid) + NX) % NX
        y = (me.y + (mid if part == 0 else large) + NY) % NY
        return self.w.at[:, y, me.k * NX + x, :, self.parts[part]]

    def slab(self, part, off):
        me = self.me
        if part == 0:
            x = (me.x + off + NX) % NX
            return self.w.at[:, :, me.k * NX + x, :, self.parts[0]]
        y = (me.y + off + NY) % NY
        return self.w.at[:, y, pl.ds(me.k * NX, NX), :, self.parts[1]]

    def peer(self, part, off):
        return self.me.xp(off) if part == 0 else self.me.yp(off)

    def core(self, ref):
        self.put(ref, self.me.other(), self.cores)

    def near(self, part, mid):
        d = self.me.d
        self.ahead[part][mid] = self.net.group()
        self.put(self.at(part, 0, mid), self.peer(part, d), self.ahead[part][mid])
        self.put(self.at(part, 0, mid), self.peer(part, -d), self.side[part])

    def middle(self):
        self.zs.wait()
        self.mids = [{j: self.net.group() for j in MID_ORDER} for part in range(2)]
        for j in MID_ORDER:
            for part in range(2):
                self.put(self.at(part, 0, 0), self.peer(1 - part, j), self.mids[part][j])
        for part in range(2):
            self.near(part, 0)

    def near_one(self):
        for j in (1, 3):
            for part in range(2):
                self.mids[part][j].wait()
                self.near(part, -j)

    def near_two(self):
        for part in range(2):
            self.mids[part][2].wait()
            self.near(part, -2)
        for part in range(2):
            self.core(self.slab(part, 0))

    def near_all(self):
        for mid in (0, -1, -3, -2):
            for part in range(2):
                self.near(part, mid)
        for part in range(2):
            self.core(self.slab(part, 0))

    def forward(self, *mids):
        d = self.me.d
        for mid in mids:
            for part in range(2):
                self.ahead[part][mid].wait()
                group = self.far[part][0 if mid in (0, -1) else 1]
                self.put(self.at(part, -d, mid), self.peer(part, d), group)
        if -2 in mids:
            for part in range(2):
                self.core(self.slab(part, -d))

    def finish(self):
        d = self.me.d
        for part in range(2):
            self.side[part].wait()
            self.core(self.slab(part, d))
        for i, mids in enumerate(((0, -1), (-3, -2))):
            for part in range(2):
                self.far[part][i].wait()
                for mid in mids:
                    self.core(self.at(part, 2, mid))

    def arrived(self):
        self.cores.wait()


class GatherRound:
    def __init__(self, net, me, w):
        self.net, self.me, self.w = net, me, w
        self.unit = net.unit()
        self.blocks, self.cores, self.last = net.group(), net.group(), net.group()
        self.up = [net.group() for step in range(3)]
        self.down = [net.group() for step in range(3)]

    def put(self, ref, peer, group):
        self.net.put(ref, ref, peer, self.unit, group)

    def plane(self):
        me = self.me
        ref = self.w.at[me.z, me.y, me.kx]
        for jy, jx in PLANE:
            self.put(ref, me.plane(jy, 0, jx), self.blocks)

    def slab(self, off):
        me = self.me
        return self.w.at[(me.z + off + NZ) % NZ, :, pl.ds(me.k * NX, NX)]

    def core(self, off):
        self.put(self.slab(off), self.me.other(), self.cores)

    def near(self):
        self.blocks.wait()
        self.put(self.slab(0), self.me.zp(1), self.up[0])
        self.put(self.slab(0), self.me.zp(-1), self.down[0])
        self.core(0)

    def step(self, i):
        self.up[i - 1].wait()
        if i < 3:
            self.put(self.slab(-i), self.me.zp(1), self.up[i])
        self.down[i - 1].wait()
        if i < 3:
            self.put(self.slab(i), self.me.zp(-1), self.down[i])
        else:
            d = self.me.d
            self.put(self.slab(-3 * d), self.me.zp(d), self.last)
        self.core(-i)
        self.core(i)

    def finish(self):
        self.last.wait()
        self.core(4)

    def arrived(self):
        self.cores.wait()


class Strips:
    def __init__(self, net, me, zb, m):
        self.net, self.me, self.zb, self.m = net, me, zb, m
        self.unit, self.zs, self.mids = net.unit(), net.group(), net.group()

    def along_z(self, block):
        me = self.me
        self.zb[me.z] = block
        ref = self.zb.at[me.z]
        for j in FAR_FIRST:
            self.net.put(ref, ref, me.zp(j), self.unit, self.zs)

    def middle(self):
        me = self.me
        half = self.m.shape[-1]
        self.zs.wait()
        for j in (2, 1, 3):
            for part, peer, own in ((0, me.yp, me.y), (1, me.xp, me.x)):
                src = self.zb.at[:, :, pl.ds(part * half, half)]
                self.net.put(src, self.m.at[part, own], peer(j), self.unit, self.mids)
        for part, own in ((0, me.y), (1, me.x)):
            self.m[part, own] = self.zb[:, :, pl.ds(part * half, half)]

    def arrived(self):
        self.mids.wait()


class Scatter:
    def __init__(self, net, me, refs):
        self.net, self.me = net, me
        (self.p, self.c, self.s, self.f, self.t, self.r, self.a, self.m, self.b, self.q) = refs
        self.unit = net.unit()
        self.cs = net.group()
        self.near = [[net.group() for mid in range(4)] for part in range(2)]
        self.far = [[net.group() for mid in range(4)] for part in range(2)]
        self.side = [net.group() for part in range(2)]
        self.mids = [net.group() for part in range(2)]
        self.zs = net.group()

    def put(self, src, dst, peer, group):
        self.net.put(src, dst, peer, self.unit, group)

    def tile(self, t, value):
        half = value.shape[1] // 2
        for y in range(NY):
            for k in range(NK):
                for x in range(NX):
                    at = ((y * NK + k) * NX + x) * BLK
                    rows = value[at : at + BLK]
                    self.p[0, k, x, y, t] = rows[:, :half].astype(BF16)
                    self.p[1, k, y, x, t] = rows[:, half:].astype(BF16)

    def cores(self, first, count):
        me = self.me
        zs = pl.ds(first, count)
        for part in range(2):
            self.put(
                self.p.at[part, 1 - me.k, :, :, zs],
                self.c.at[part, :, :, zs],
                me.other(),
                self.cs,
            )

    def peer(self, part, off):
        return self.me.xp(off) if part == 0 else self.me.yp(off)

    def index(self, part, off):
        return (self.me.x + off + NX) % NX if part == 0 else (self.me.y + off + NY) % NY

    def joined(self, part, off, mid):
        at, i = self.index(part, off), self.index(1 - part, mid)
        total = self.p[part, self.me.k, at, i].astype(F32) + self.c[part, at, i].astype(F32)
        self.s[part, at, i] = total.astype(BF16)
        return self.s.at[part, at, i]

    def large(self):
        d = self.me.d
        self.cs.wait()
        for mid in STRIPS:
            for part in range(2):
                dst = self.f.at[part, self.index(1 - part, mid)]
                src = self.joined(part, 2, mid)
                self.put(src, dst, self.peer(part, d), self.near[part][mid])
        for mid in STRIPS:
            for part in range(2):
                dst = self.r.at[part, 0, self.index(1 - part, mid)]
                src = self.joined(part, -d, mid)
                self.put(src, dst, self.peer(part, -d), self.side[part])
        for mid in STRIPS:
            for part in range(2):
                self.joined(part, d, mid)
                self.joined(part, 0, mid)

    def forward(self):
        d = self.me.d
        for mid in STRIPS:
            for part in range(2):
                self.near[part][mid].wait()
                i = self.index(1 - part, mid)
                total = self.s[part, self.index(part, d), i].astype(F32)
                total = total + self.f[part, i].astype(F32)
                self.t[part, i] = total.astype(BF16)
                dst = self.r.at[part, 1, i]
                self.put(self.t.at[part, i], dst, self.peer(part, d), self.far[part][mid])

    def middle(self):
        for part in range(2):
            self.side[part].wait()
        for mid in STRIPS:
            for part in range(2):
                self.far[part][mid].wait()
                i = self.index(1 - part, mid)
                total = self.s[part, self.index(part, 0), i].astype(F32)
                total = total + self.r[part, 0, i].astype(F32)
                total = total + self.r[part, 1, i].astype(F32)
                self.a[part, i] = total.astype(BF16)
                if mid:
                    dst = self.m.at[part, mid - 1]
                    self.put(self.a.at[part, i], dst, self.peer(1 - part, mid), self.mids[part])

    def along_z(self):
        me = self.me
        for part in range(2):
            self.mids[part].wait()
            at = self.index(1 - part, 0)
            total = self.a[part, at].astype(F32)
            for j in range(3):
                total = total + self.m[part, j].astype(F32)
            half = total.shape[-1]
            self.b[:, :, pl.ds(part * half, half)] = total.astype(BF16)
        for j in FAR_FIRST:
            self.put(self.b.at[(me.z + j) % NZ], self.q.at[j - 1], me.zp(j), self.zs)

    def result(self):
        self.zs.wait()
        total = self.b[self.me.z].astype(F32)
        for j in range(7):
            total = total + self.q[j].astype(F32)
        return total


class Norms:
    def __init__(self, net, me, refs):
        self.net, self.me, self.refs = net, me, refs
        self.unit = net.unit()
        self.groups = [net.group() for axis in range(2)]

    def start(self, axis, row):
        me = self.me
        ref = self.refs[axis]
        own = me.gy * NX + me.x if axis else me.z
        ref[own] = row
        peers = [me.zp(j) for j in FAR_FIRST]
        if axis:
            peers = [me.plane(jy, 1, jx) for jy, jx in PLANE]
            peers += [me.plane(jy, 0, jx) for jy, jx in PLANE] + [me.other()]
        for peer in peers:
            self.net.put(ref.at[own], ref.at[own], peer, self.unit, self.groups[axis])

    def finish(self, axis):
        ref = self.refs[axis]
        self.wait(self.groups[axis].sem, ref.shape[0] - 1)
        total = ref[0]
        for i in range(1, ref.shape[0]):
            total = total + ref[i]
        return total

    def wait(self, sem, count):
        ref = self.refs[2].at[pl.ds(0, count)]
        pltpu.make_async_copy(ref, ref, sem).wait()

    def sent(self):
        self.wait(self.unit.sem, NZ + NY * NX * NK - 2)


def fold(sq):
    lanes = sq[:, 0:128]
    for i in range(1, sq.shape[1] // 128):
        lanes = lanes + sq[:, 128 * i : 128 * (i + 1)]
    row = jnp.sum(lanes, axis=0, keepdims=True)
    return row + pltpu.roll(row, 64, 1)


def low_lanes():
    return lax.broadcasted_iota(jnp.int32, (1, 128), 1) < 64


def stat_row(w, g):
    return jnp.where(low_lanes(), fold(w * w), fold(g * g))


def trust_of(row):
    wsquare = jnp.sum(jnp.where(low_lanes(), row, 0.0), axis=1, keepdims=True)
    gsquare = jnp.sum(jnp.where(low_lanes(), 0.0, row), axis=1, keepdims=True)
    wnorm = jnp.sqrt(wsquare)
    gnorm = jnp.sqrt(gsquare)
    return wnorm / (gnorm + 5e-05 * wnorm)


def updated(master, grads, velocity, trust):
    new_velocity = 0.9 * velocity + trust * (grads + 5e-05 * master)
    new_master = master - 0.1 * new_velocity
    return new_master, new_velocity


def kernel(
    acts_h, hid_h, go_h, mr_h, me_h, vr_h, ve_h,
    gi, smallout, ne, nr,
    acts, hid, go, small, gh, acc,
    we, wr, flat, g_kept, az, am, gz, gm, ge_refs, gr_refs, nz_e, nz_r,
    send, recv, load, spare,
):
    scope = jax.named_scope
    me = Place()
    net = Net(send, recv, spare)
    channels = go.shape[1]
    middle = hid.shape[1]
    half = middle // 2
    inv_c = 1.0 / float(channels) ** 0.5
    inv_m = 1.0 / float(middle) ** 0.5

    loads = [
        pltpu.make_async_copy(src, dst, load.at[i])
        for i, (src, dst) in enumerate(
            (
                (me_h, small.at[0]),
                (mr_h, small.at[1]),
                (vr_h, small.at[3]),
                (ve_h, small.at[2]),
                (go_h, go),
                (hid_h, hid),
                (acts_h, acts),
            )
        )
    ]
    for copy in loads:
        copy.start()

    barrier = pltpu.get_barrier_semaphore()
    peers = [me.zp(j) for j in FAR_FIRST] + [me.other()]
    peers += [me.plane(jy, jk, jx) for jk in range(NK) for jy, jx in PLANE]
    for peer in peers:
        pl.semaphore_signal(barrier, inc=1, device_id=peer, device_id_type=MESH)

    for copy in loads[:4]:
        copy.wait()
    we[me.z, me.y, me.kx] = small[0].astype(BF16)
    wr[me.z, me.y, me.kx] = small[1].astype(BF16)
    with scope("barrier"):
        pl.semaphore_wait(barrier, len(peers))

    gather_e = Gather(net, me, we)
    gather_r = GatherRound(net, me, wr)
    gather_ne = Gather(net, me, ne)
    gather_nr = Gather(net, me, nr)
    scatter_e = Scatter(net, me, ge_refs)
    scatter_r = Scatter(net, me, gr_refs)
    norms_e = Norms(net, me, nz_e)
    norms_r = Norms(net, me, nz_r)
    strips_a = Strips(net, me, az, am)
    strips_g = Strips(net, me, gz, gm)
    tiles = channels // 256

    def tile_cols(t):
        return pl.ds(pl.multiple_of(t * 256, 256), 256)

    def natural(w, t):
        block = w[t].reshape(NY * NK * NX, BLK, middle)
        return block.astype(F32).reshape(256, middle).astype(BF16)

    def ge_tile(t, carry):
        value = lax.dot_general(
            go[:, tile_cols(t)], hid[...], (((0,), (0,)), ((), ())), preferred_element_type=F32
        )
        scatter_e.tile(t, value * inv_m)
        return carry

    def gr_tile(t, carry):
        value = lax.dot_general(
            acts[:, tile_cols(t)], gh[...], (((0,), (0,)), ((), ())), preferred_element_type=F32
        )
        scatter_r.tile(t, value * inv_c)
        return carry

    def flatten(t, carry):
        flat[tile_cols(t), :] = natural(we, t)
        return carry

    def gi_tile(t, carry):
        cols = tile_cols(t)
        back = lax.dot_general(
            gh[...], natural(wr, t), (((1,), (1,)), ((), ())), preferred_element_type=F32
        )
        gi[:, cols] = (go[:, cols].astype(F32) + back * inv_c).astype(BF16)
        return carry

    def e_result():
        g = scatter_e.result()
        g_kept[0] = g
        norms_e.start(0, stat_row(small[0], g))

    def r_result():
        g = scatter_r.result()
        g_kept[1] = g
        norms_r.start(0, stat_row(small[1], g))
        strips_g.along_z((g + 5e-05 * small[1]).astype(BF16))

    def norm_step(norms, axis):
        norms.start(axis + 1, norms.finish(axis))

    def e_update():
        trust = trust_of(norms_e.finish(1))
        new_master, new_velocity = updated(small[0], g_kept[0], small[2], trust)
        ne[me.z, me.y, me.kx] = new_master.astype(BF16)
        gather_ne.along_z()
        smallout[0] = new_master
        smallout[1] = new_velocity

    def r_update():
        trust = trust_of(norms_r.finish(1))
        strips_g.arrived()
        step = jnp.broadcast_to(0.1 * trust, (BLK, half))

        def fill(i, carry):
            for z in range(NZ):
                for part in range(2):
                    block = am[part, i, z] - step * gm[part, i, z].astype(F32)
                    if part == 0:
                        nr[z, i, me.kx, :, pl.ds(0, half)] = block.astype(BF16)
                    else:
                        nr[z, me.y, me.k * NX + i, :, pl.ds(half, half)] = block.astype(BF16)
            return carry

        lax.fori_loop(0, 4, fill, 0)
        gather_nr.near_all()
        new_master, new_velocity = updated(small[1], g_kept[1], small[3], trust)
        smallout[2] = new_master
        smallout[3] = new_velocity

    def ge_part(first, count):
        lax.fori_loop(first, first + count, ge_tile, 0)
        scatter_e.cores(first, count)

    def gr_part(first, count):
        lax.fori_loop(first, first + count, gr_tile, 0)
        scatter_r.cores(first, count)

    def hidden():
        lax.fori_loop(0, tiles, flatten, 0)
        acc[...] = jnp.dot(go[...], flat[...], preferred_element_type=F32)
        gh[...] = jnp.where(hid[...].astype(F32) > 0, acc[...] * inv_m, 0.0).astype(BF16)

    program = [
        ("E z", gather_e.along_z),
        ("R plane", gather_r.plane),
        ("load go", loads[4].wait),
        ("load hid", loads[5].wait),
        ("GE tiles 0", lambda: ge_part(0, 4)),
        ("GE tiles 1", lambda: ge_part(4, 4)),
        ("E mid", gather_e.middle),
        ("A z", lambda: strips_a.along_z(small[1] - 0.09 * small[3])),
        ("E near 1", gather_e.near_one),
        ("R near", gather_r.near),
        ("E fwd 0", lambda: gather_e.forward(0)),
        ("E near 2", gather_e.near_two),
        ("E fwd 1", lambda: gather_e.forward(-1, -3)),
        ("E fwd 2", lambda: gather_e.forward(-2)),
        ("GE large", scatter_e.large),
        ("E finish", gather_e.finish),
        ("R step 1", lambda: gather_r.step(1)),
        ("E arrived", gather_e.arrived),
        ("hidden", hidden),
        ("A mid", strips_a.middle),
        ("GE forward", scatter_e.forward),
        ("load acts", loads[6].wait),
        ("GR tiles 0", lambda: gr_part(0, 4)),
        ("R step 2", lambda: gather_r.step(2)),
        ("GR tiles 1", lambda: gr_part(4, 4)),
        ("GE mid", scatter_e.middle),
        ("GR large", scatter_r.large),
        ("GE z", scatter_e.along_z),
        ("GR forward", scatter_r.forward),
        ("R step 3", lambda: gather_r.step(3)),
        ("GR mid", scatter_r.middle),
        ("GE result", e_result),
        ("GR z", scatter_r.along_z),
        ("R finish", gather_r.finish),
        ("norm e", lambda: norm_step(norms_e, 0)),
        ("R arrived", gather_r.arrived),
        ("GR result", r_result),
        ("A arrived", strips_a.arrived),
        ("gi", lambda: lax.fori_loop(0, tiles, gi_tile, 0)),
        ("E update", e_update),
        ("norm r", lambda: norm_step(norms_r, 0)),
        ("g mid", strips_g.middle),
        ("NE mid", gather_ne.middle),
        ("R update", r_update),
        ("NE near 1", gather_ne.near_one),
        ("NE fwd 0", lambda: gather_ne.forward(0)),
        ("NE near 2", gather_ne.near_two),
        ("NR fwd", lambda: gather_nr.forward(0, -1, -3, -2)),
        ("NE fwd 1", lambda: gather_ne.forward(-1, -3, -2)),
        ("NR finish", gather_nr.finish),
        ("NE finish", gather_ne.finish),
        ("NR arrived", gather_nr.arrived),
        ("NE arrived", gather_ne.arrived),
    ]
    for name, step in program:
        with scope(name.replace(" ", "_")):
            step()
    with scope("drain"):
        for unit in (
            gather_e, gather_r, gather_ne, gather_nr, scatter_e, scatter_r,
            strips_a, strips_g,
        ):
            unit.unit.wait()
        norms_e.sent()
        norms_r.sent()
    assert (net.units, net.used) == (SENDS, RECVS)


def write_out(gi, small, ne, nr, gi_h, nmr_h, nme_h, nvr_h, nve_h, wr_h, we_h, sem):
    copies = [
        pltpu.make_async_copy(src, dst, sem.at[i])
        for i, (src, dst) in enumerate(
            (
                (gi, gi_h),
                (ne, we_h),
                (nr, wr_h),
                (small.at[0], nme_h),
                (small.at[1], nve_h),
                (small.at[2], nmr_h),
                (small.at[3], nvr_h),
            )
        )
    ]
    for copy in copies:
        copy.start()
    for copy in copies:
        copy.wait()


def shards(acts, hid, go, mr, me_, vr, ve):
    rows, channels = acts.shape
    middle = hid.shape[1]
    half = middle // 2
    own = mr.shape
    whole = (NZ, NY, NK * NX, BLK, middle)
    scatter = (
        pltpu.VMEM((2, NK, 4, 4, NZ, BLK, half), BF16),
        pltpu.VMEM((2, 4, 4, NZ, BLK, half), BF16),
        pltpu.VMEM((2, 4, 4, NZ, BLK, half), BF16),
        pltpu.VMEM((2, 4, NZ, BLK, half), BF16),
        pltpu.VMEM((2, 4, NZ, BLK, half), BF16),
        pltpu.VMEM((2, 2, 4, NZ, BLK, half), BF16),
        pltpu.VMEM((2, 4, NZ, BLK, half), BF16),
        pltpu.VMEM((2, 3, NZ, BLK, half), BF16),
        pltpu.VMEM((NZ, BLK, middle), BF16),
        pltpu.VMEM((NZ - 1, BLK, middle), BF16),
    )
    norms = tuple(pltpu.VMEM((n, 1, 128), F32) for n in (NZ, NY * NX * NK, 40))
    in_hbm = pl.BlockSpec(memory_space=pltpu.HBM)
    vmem = pl.BlockSpec(memory_space=pltpu.VMEM)
    args = [pltpu.with_memory_space_constraint(a, pltpu.HBM) for a in (acts, hid, go, mr, me_, vr, ve)]
    results = pl.pallas_call(
        kernel,
        out_shape=(
            pltpu.VMEM((rows, channels), BF16),
            pltpu.VMEM((4, *own), F32),
            pltpu.VMEM(whole, BF16),
            pltpu.VMEM(whole, BF16),
        ),
        in_specs=[in_hbm] * 7,
        out_specs=(vmem,) * 4,
        scratch_shapes=[
            pltpu.VMEM((rows, channels), BF16),
            pltpu.VMEM((rows, middle), BF16),
            pltpu.VMEM((rows, channels), BF16),
            pltpu.VMEM((4, *own), F32),
            pltpu.VMEM((rows, middle), BF16),
            pltpu.VMEM((rows, middle), F32),
            pltpu.VMEM(whole, BF16),
            pltpu.VMEM(whole, BF16),
            pltpu.VMEM((channels, middle), BF16),
            pltpu.VMEM((2, *own), F32),
            pltpu.VMEM((NZ, BLK, middle), F32),
            pltpu.VMEM((2, 4, NZ, BLK, half), F32),
            pltpu.VMEM((NZ, BLK, middle), BF16),
            pltpu.VMEM((2, 4, NZ, BLK, half), BF16),
            scatter,
            scatter,
            norms,
            norms,
            pltpu.SemaphoreType.DMA((SENDS,)),
            pltpu.SemaphoreType.DMA((RECVS,)),
            pltpu.SemaphoreType.DMA((7,)),
            pltpu.VMEM((512, BLK, half), BF16),
        ],
        compiler_params=pltpu.CompilerParams(
            collective_id=0, has_side_effects=True, vmem_limit_bytes=44 * 1024 * 1024
        ),
    )(*args)
    out = pl.pallas_call(
        write_out,
        out_shape=(
            jax.ShapeDtypeStruct((rows, channels), BF16),
            jax.ShapeDtypeStruct(own, F32),
            jax.ShapeDtypeStruct(own, F32),
            jax.ShapeDtypeStruct(own, F32),
            jax.ShapeDtypeStruct(own, F32),
            jax.ShapeDtypeStruct(whole, BF16),
            jax.ShapeDtypeStruct(whole, BF16),
        ),
        in_specs=[vmem] * 4,
        out_specs=(in_hbm,) * 7,
        scratch_shapes=[pltpu.SemaphoreType.DMA((7,))],
        compiler_params=pltpu.CompilerParams(vmem_limit_bytes=4 * 1024 * 1024),
    )(*results)
    flat = (channels, middle)
    return (*out[:5], out[5].reshape(flat), out[6].reshape(flat))


def solution(mesh):
    split = P(ROWS_SPLIT, None)
    return jax.shard_map(
        shards,
        mesh=mesh,
        in_specs=(split,) * 7,
        out_specs=(split,) * 5 + (P(), P()),
        check_vma=False,
    )
```

```python
import jax
import jax.numpy as jnp
from jax import lax
from jax.experimental import pallas as pl
from jax.experimental.pallas import tpu as pltpu
from jax.sharding import PartitionSpec as P

MESH = pl.DeviceIdType.MESH
BF16 = jnp.bfloat16
F32 = jnp.float32
ROWS_SPLIT = ("gx", "gy", "gz")
NZ, NY, NX, NK = 8, 4, 4, 2
BLK = 8
FAR_FIRST = (4, 3, 5, 2, 6, 1, 7)
STRIPS = (2, 1, 3, 0)
PLANE = [(jy, jx) for jy in (2, 1, 3, 0) for jx in (2, 1, 3, 0)][:-1]
SENDS = 12
RECVS = 117
MID_ORDER = (1, 3, 2)


class Group:
    def __init__(self, net, sem):
        self.net, self.sem, self.bytes = net, sem, 0

    def wait(self):
        self.net.wait(self.sem, self.bytes)


class Net:
    def __init__(self, send, recv, spare):
        self.send, self.recv, self.spare = send, recv, spare
        self.used = self.units = 0

    def unit(self):
        self.units += 1
        return Group(self, self.send.at[self.units - 1])

    def group(self):
        self.used += 1
        return Group(self, self.recv.at[self.used - 1])

    def put(self, src, dst, peer, unit, group):
        size = src.dtype.itemsize
        for extent in src.shape:
            size *= extent
        unit.bytes += size
        group.bytes += size
        pltpu.make_async_remote_copy(
            src_ref=src,
            dst_ref=dst,
            send_sem=unit.sem,
            recv_sem=group.sem,
            device_id=peer,
            device_id_type=MESH,
        ).start()

    def wait(self, sem, size):
        blocks, rest = divmod(size, 4096)
        assert rest == 0
        ref = self.spare.at[pl.ds(0, blocks)]
        pltpu.make_async_copy(ref, ref, sem).wait()


class Place:
    def __init__(self):
        self.z = lax.axis_index("gx")
        gy = lax.axis_index("gy")
        self.y = gy // 2
        self.k = gy % 2
        self.x = lax.axis_index("gz")
        self.gy = gy
        self.kx = self.k * NX + self.x
        self.d = 1 - 2 * self.k

    def zp(self, j):
        return {"gx": (self.z + j + NZ) % NZ}

    def plane(self, jy, jk, jx):
        y = (self.y + jy) % NY
        return {"gy": y * NK + (self.k + jk) % NK, "gz": (self.x + jx) % NX}

    def yp(self, j):
        return {"gy": ((self.y + j + NY) % NY) * 2 + self.k}

    def xp(self, j):
        return {"gz": (self.x + j + NX) % NX}

    def other(self):
        return {"gy": self.gy + 1 - 2 * self.k}


class Gather:
    def __init__(self, net, me, w):
        self.net, self.me, self.w = net, me, w
        half = w.shape[-1] // 2
        self.parts = (pl.ds(0, half), pl.ds(half, half))
        self.unit = net.unit()
        self.cores = net.group()
        self.ahead = ({}, {})
        self.side = [net.group() for part in range(2)]
        self.far = [[net.group(), net.group()] for part in range(2)]

    def put(self, ref, peer, group):
        self.net.put(ref, ref, peer, self.unit, group)

    def along_z(self):
        me = self.me
        ref = self.w.at[me.z, me.y, me.kx]
        self.zs = self.net.group()
        for j in FAR_FIRST:
            self.put(ref, me.zp(j), self.zs)

    def at(self, part, large, mid):
        me = self.me
        x = (me.x + (large if part == 0 else mid) + NX) % NX
        y = (me.y + (mid if part == 0 else large) + NY) % NY
        return self.w.at[:, y, me.k * NX + x, :, self.parts[part]]

    def slab(self, part, off):
        me = self.me
        if part == 0:
            x = (me.x + off + NX) % NX
            return self.w.at[:, :, me.k * NX + x, :, self.parts[0]]
        y = (me.y + off + NY) % NY
        return self.w.at[:, y, pl.ds(me.k * NX, NX), :, self.parts[1]]

    def peer(self, part, off):
        return self.me.xp(off) if part == 0 else self.me.yp(off)

    def core(self, ref):
        self.put(ref, self.me.other(), self.cores)

    def near(self, part, mid):
        d = self.me.d
        self.ahead[part][mid] = self.net.group()
        self.put(self.at(part, 0, mid), self.peer(part, d), self.ahead[part][mid])
        self.put(self.at(part, 0, mid), self.peer(part, -d), self.side[part])

    def middle(self):
        self.zs.wait()
        self.mids = [{j: self.net.group() for j in MID_ORDER} for part in range(2)]
        for j in MID_ORDER:
            for part in range(2):
                self.put(self.at(part, 0, 0), self.peer(1 - part, j), self.mids[part][j])
        for part in range(2):
            self.near(part, 0)

    def near_one(self):
        for j in (1, 3):
            for part in range(2):
                self.mids[part][j].wait()
                self.near(part, -j)

    def near_two(self):
        for part in range(2):
            self.mids[part][2].wait()
            self.near(part, -2)
        for part in range(2):
            self.core(self.slab(part, 0))

    def near_all(self):
        for mid in (0, -1, -3, -2):
            for part in range(2):
                self.near(part, mid)
        for part in range(2):
            self.core(self.slab(part, 0))

    def forward(self, *mids):
        d = self.me.d
        for mid in mids:
            for part in range(2):
                self.ahead[part][mid].wait()
                group = self.far[part][0 if mid in (0, -1) else 1]
                self.put(self.at(part, -d, mid), self.peer(part, d), group)
        if -2 in mids:
            for part in range(2):
                self.core(self.slab(part, -d))

    def finish(self):
        d = self.me.d
        for part in range(2):
            self.side[part].wait()
            self.core(self.slab(part, d))
        for i, mids in enumerate(((0, -1), (-3, -2))):
            for part in range(2):
                self.far[part][i].wait()
                for mid in mids:
                    self.core(self.at(part, 2, mid))

    def arrived(self):
        self.cores.wait()


class GatherRound:
    def __init__(self, net, me, w):
        self.net, self.me, self.w = net, me, w
        self.unit = net.unit()
        self.blocks, self.cores, self.last = net.group(), net.group(), net.group()
        self.up = [net.group() for step in range(3)]
        self.down = [net.group() for step in range(3)]

    def put(self, ref, peer, group):
        self.net.put(ref, ref, peer, self.unit, group)

    def plane(self):
        me = self.me
        ref = self.w.at[me.z, me.y, me.kx]
        for jy, jx in PLANE:
            self.put(ref, me.plane(jy, 0, jx), self.blocks)

    def slab(self, off):
        me = self.me
        return self.w.at[(me.z + off + NZ) % NZ, :, pl.ds(me.k * NX, NX)]

    def core(self, off):
        self.put(self.slab(off), self.me.other(), self.cores)

    def near(self):
        self.blocks.wait()
        self.put(self.slab(0), self.me.zp(1), self.up[0])
        self.put(self.slab(0), self.me.zp(-1), self.down[0])
        self.core(0)

    def step(self, i):
        self.up[i - 1].wait()
        if i < 3:
            self.put(self.slab(-i), self.me.zp(1), self.up[i])
        self.down[i - 1].wait()
        if i < 3:
            self.put(self.slab(i), self.me.zp(-1), self.down[i])
        else:
            d = self.me.d
            self.put(self.slab(-3 * d), self.me.zp(d), self.last)
        self.core(-i)
        self.core(i)

    def finish(self):
        self.last.wait()
        self.core(4)

    def arrived(self):
        self.cores.wait()


class Strips:
    def __init__(self, net, me, zb, m):
        self.net, self.me, self.zb, self.m = net, me, zb, m
        self.unit, self.zs, self.mids = net.unit(), net.group(), net.group()

    def along_z(self, block):
        me = self.me
        self.zb[me.z] = block
        ref = self.zb.at[me.z]
        for j in FAR_FIRST:
            self.net.put(ref, ref, me.zp(j), self.unit, self.zs)

    def middle(self):
        me = self.me
        half = self.m.shape[-1]
        self.zs.wait()
        for j in (2, 1, 3):
            for part, peer, own in ((0, me.yp, me.y), (1, me.xp, me.x)):
                src = self.zb.at[:, :, pl.ds(part * half, half)]
                self.net.put(src, self.m.at[part, own], peer(j), self.unit, self.mids)
        for part, own in ((0, me.y), (1, me.x)):
            self.m[part, own] = self.zb[:, :, pl.ds(part * half, half)]

    def arrived(self):
        self.mids.wait()


class Scatter:
    def __init__(self, net, me, refs):
        self.net, self.me = net, me
        (self.p, self.c, self.s, self.f, self.t, self.r, self.a, self.m, self.b, self.q) = refs
        self.unit = net.unit()
        self.cs = net.group()
        self.near = [[net.group() for mid in range(4)] for part in range(2)]
        self.far = [[net.group() for mid in range(4)] for part in range(2)]
        self.side = [net.group() for part in range(2)]
        self.mids = [net.group() for part in range(2)]
        self.zs = net.group()

    def put(self, src, dst, peer, group):
        self.net.put(src, dst, peer, self.unit, group)

    def tile(self, t, value):
        half = value.shape[1] // 2
        for y in range(NY):
            for k in range(NK):
                for x in range(NX):
                    at = ((y * NK + k) * NX + x) * BLK
                    rows = value[at : at + BLK]
                    self.p[0, k, x, y, t] = rows[:, :half].astype(BF16)
                    self.p[1, k, y, x, t] = rows[:, half:].astype(BF16)

    def cores(self, first, count):
        me = self.me
        zs = pl.ds(first, count)
        for part in range(2):
            self.put(
                self.p.at[part, 1 - me.k, :, :, zs],
                self.c.at[part, :, :, zs],
                me.other(),
                self.cs,
            )

    def peer(self, part, off):
        return self.me.xp(off) if part == 0 else self.me.yp(off)

    def index(self, part, off):
        return (self.me.x + off + NX) % NX if part == 0 else (self.me.y + off + NY) % NY

    def joined(self, part, off, mid):
        at, i = self.index(part, off), self.index(1 - part, mid)
        total = self.p[part, self.me.k, at, i].astype(F32) + self.c[part, at, i].astype(F32)
        self.s[part, at, i] = total.astype(BF16)
        return self.s.at[part, at, i]

    def large(self):
        d = self.me.d
        self.cs.wait()
        for mid in STRIPS:
            for part in range(2):
                dst = self.f.at[part, self.index(1 - part, mid)]
                src = self.joined(part, 2, mid)
                self.put(src, dst, self.peer(part, d), self.near[part][mid])

    def aside(self):
        d = self.me.d
        for mid in STRIPS:
            for part in range(2):
                dst = self.r.at[part, 0, self.index(1 - part, mid)]
                src = self.joined(part, -d, mid)
                self.put(src, dst, self.peer(part, -d), self.side[part])
        for mid in STRIPS:
            for part in range(2):
                self.joined(part, d, mid)
                self.joined(part, 0, mid)

    def forward(self):
        d = self.me.d
        for mid in STRIPS:
            for part in range(2):
                self.near[part][mid].wait()
                i = self.index(1 - part, mid)
                total = self.s[part, self.index(part, d), i].astype(F32)
                total = total + self.f[part, i].astype(F32)
                self.t[part, i] = total.astype(BF16)
                dst = self.r.at[part, 1, i]
                self.put(self.t.at[part, i], dst, self.peer(part, d), self.far[part][mid])

    def middle(self):
        for part in range(2):
            self.side[part].wait()
        for mid in STRIPS:
            for part in range(2):
                self.far[part][mid].wait()
                i = self.index(1 - part, mid)
                total = self.s[part, self.index(part, 0), i].astype(F32)
                total = total + self.r[part, 0, i].astype(F32)
                total = total + self.r[part, 1, i].astype(F32)
                self.a[part, i] = total.astype(BF16)
                if mid:
                    dst = self.m.at[part, mid - 1]
                    self.put(self.a.at[part, i], dst, self.peer(1 - part, mid), self.mids[part])

    def along_z(self):
        me = self.me
        for part in range(2):
            self.mids[part].wait()
            at = self.index(1 - part, 0)
            total = self.a[part, at].astype(F32)
            for j in range(3):
                total = total + self.m[part, j].astype(F32)
            half = total.shape[-1]
            self.b[:, :, pl.ds(part * half, half)] = total.astype(BF16)
        for j in FAR_FIRST:
            self.put(self.b.at[(me.z + j) % NZ], self.q.at[j - 1], me.zp(j), self.zs)

    def result(self):
        self.zs.wait()
        total = self.b[self.me.z].astype(F32)
        for j in range(7):
            total = total + self.q[j].astype(F32)
        return total


class Norms:
    def __init__(self, net, me, refs):
        self.net, self.me, self.refs = net, me, refs
        self.unit = net.unit()
        self.groups = [net.group() for axis in range(2)]

    def start(self, axis, row):
        me = self.me
        ref = self.refs[axis]
        own = me.gy * NX + me.x if axis else me.z
        ref[own] = row
        peers = [me.zp(j) for j in FAR_FIRST]
        if axis:
            peers = [me.plane(jy, 1, jx) for jy, jx in PLANE]
            peers += [me.plane(jy, 0, jx) for jy, jx in PLANE] + [me.other()]
        for peer in peers:
            self.net.put(ref.at[own], ref.at[own], peer, self.unit, self.groups[axis])

    def finish(self, axis):
        ref = self.refs[axis]
        self.wait(self.groups[axis].sem, ref.shape[0] - 1)
        total = ref[0]
        for i in range(1, ref.shape[0]):
            total = total + ref[i]
        return total

    def wait(self, sem, count):
        ref = self.refs[2].at[pl.ds(0, count)]
        pltpu.make_async_copy(ref, ref, sem).wait()

    def sent(self):
        self.wait(self.unit.sem, NZ + NY * NX * NK - 2)


def fold(sq):
    lanes = sq[:, 0:128]
    for i in range(1, sq.shape[1] // 128):
        lanes = lanes + sq[:, 128 * i : 128 * (i + 1)]
    row = jnp.sum(lanes, axis=0, keepdims=True)
    return row + pltpu.roll(row, 64, 1)


def low_lanes():
    return lax.broadcasted_iota(jnp.int32, (1, 128), 1) < 64


def stat_row(w, g):
    return jnp.where(low_lanes(), fold(w * w), fold(g * g))


def trust_of(row):
    wsquare = jnp.sum(jnp.where(low_lanes(), row, 0.0), axis=1, keepdims=True)
    gsquare = jnp.sum(jnp.where(low_lanes(), 0.0, row), axis=1, keepdims=True)
    wnorm = jnp.sqrt(wsquare)
    gnorm = jnp.sqrt(gsquare)
    return wnorm / (gnorm + 5e-05 * wnorm)


def updated(master, grads, velocity, trust):
    new_velocity = 0.9 * velocity + trust * (grads + 5e-05 * master)
    new_master = master - 0.1 * new_velocity
    return new_master, new_velocity


def kernel(
    acts_h, hid_h, go_h, mr_h, me_h, vr_h, ve_h,
    gi, smallout, ne, nr,
    acts, hid, go, small, gh, acc,
    we, wr, flat, g_kept, az, am, gz, gm, turned, ge_refs, gr_refs, nz_e, nz_r,
    send, recv, load, spare,
):
    scope = jax.named_scope
    me = Place()
    net = Net(send, recv, spare)
    channels = go.shape[1]
    middle = hid.shape[1]
    half = middle // 2
    inv_c = 1.0 / float(channels) ** 0.5
    inv_m = 1.0 / float(middle) ** 0.5

    loads = [
        pltpu.make_async_copy(src, dst, load.at[i])
        for i, (src, dst) in enumerate(
            (
                (me_h, small.at[0]),
                (mr_h, small.at[1]),
                (vr_h, small.at[3]),
                (ve_h, small.at[2]),
                (go_h, go),
                (hid_h, hid),
                (acts_h, acts),
            )
        )
    ]
    for copy in loads:
        copy.start()

    barrier = pltpu.get_barrier_semaphore()
    peers = [me.zp(j) for j in FAR_FIRST] + [me.other()]
    peers += [me.plane(jy, jk, jx) for jk in range(NK) for jy, jx in PLANE]
    for peer in peers:
        pl.semaphore_signal(barrier, inc=1, device_id=peer, device_id_type=MESH)

    for copy in loads[:4]:
        copy.wait()
    we[me.z, me.y, me.kx] = small[0].astype(BF16)
    wr[me.z, me.y, me.kx] = small[1].astype(BF16)
    with scope("barrier"):
        pl.semaphore_wait(barrier, len(peers))

    gather_e = Gather(net, me, we)
    gather_r = GatherRound(net, me, wr)
    gather_ne = Gather(net, me, ne)
    gather_nr = Gather(net, me, nr)
    scatter_e = Scatter(net, me, ge_refs)
    scatter_r = Scatter(net, me, gr_refs)
    norms_e = Norms(net, me, nz_e)
    norms_r = Norms(net, me, nz_r)
    strips_ae = Strips(net, me, az.at[0], am.at[0])
    strips_ar = Strips(net, me, az.at[1], am.at[1])
    strips_ge = Strips(net, me, gz.at[0], gm.at[0])
    strips_gr = Strips(net, me, gz.at[1], gm.at[1])
    tiles = channels // 256

    def tile_cols(t):
        return pl.ds(pl.multiple_of(t * 256, 256), 256)

    def natural(w, t):
        block = w[t].reshape(NY * NK * NX, BLK, middle)
        return block.astype(F32).reshape(256, middle).astype(BF16)

    def ge_tile(t, carry):
        value = lax.dot_general(
            go[:, tile_cols(t)], hid[...], (((0,), (0,)), ((), ())), preferred_element_type=F32
        )
        scatter_e.tile(t, value * inv_m)
        return carry

    def gr_tile(t, carry):
        value = jnp.dot(turned[tile_cols(t), :], gh[...], preferred_element_type=F32)
        scatter_r.tile(t, value * inv_c)
        return carry

    def flatten(t, carry):
        flat[tile_cols(t), :] = natural(we, t)
        return carry

    def gi_tile(t, carry):
        cols = tile_cols(t)
        back = lax.dot_general(
            gh[...], natural(wr, t), (((1,), (1,)), ((), ())), preferred_element_type=F32
        )
        gi[:, cols] = (go[:, cols].astype(F32) + back * inv_c).astype(BF16)
        return carry

    def far_term(i):
        return (small[i] - 0.09 * small[i + 2]).astype(BF16)

    def result(i, scatter, norms, strips):
        g = scatter.result()
        g_kept[i] = g
        norms.start(0, stat_row(small[i], g))
        strips.along_z((g + 5e-05 * small[i]).astype(BF16))

    def norm_step(norms):
        norms.start(1, norms.finish(0))

    def update(i, out, norms, strips, gather):
        trust = trust_of(norms.finish(1))
        strips.arrived()
        step = jnp.broadcast_to(0.1 * trust, (BLK, half))

        def fill(at, carry):
            for z in range(NZ):
                for part in range(2):
                    block = am[i, part, at, z].astype(F32) - step * gm[i, part, at, z].astype(F32)
                    if part == 0:
                        out[z, at, me.kx, :, pl.ds(0, half)] = block.astype(BF16)
                    else:
                        out[z, me.y, me.k * NX + at, :, pl.ds(half, half)] = block.astype(BF16)
            return carry

        lax.fori_loop(0, 4, fill, 0)
        gather.near_all()
        new_master, new_velocity = updated(small[i], g_kept[i], small[i + 2], trust)
        smallout[2 * i] = new_master
        smallout[2 * i + 1] = new_velocity

    def turn(first, count):
        def one(t, carry):
            turned[tile_cols(t), :] = acts[:, tile_cols(t)].T
            return carry

        lax.fori_loop(first, first + count, one, 0)

    def ge_part(first, count):
        lax.fori_loop(first, first + count, ge_tile, 0)
        scatter_e.cores(first, count)

    def gr_part(first, count):
        lax.fori_loop(first, first + count, gr_tile, 0, unroll=True)
        scatter_r.cores(first, count)

    def hidden():
        lax.fori_loop(0, tiles, flatten, 0)
        acc[...] = jnp.dot(go[...], flat[...], preferred_element_type=F32)
        gh[...] = jnp.where(hid[...].astype(F32) > 0, acc[...] * inv_m, 0.0).astype(BF16)

    program = [
        ("E z", gather_e.along_z),
        ("R plane", gather_r.plane),
        ("load go", loads[4].wait),
        ("load hid", loads[5].wait),
        ("GE tiles 0", lambda: ge_part(0, 4)),
        ("GE tiles 1", lambda: ge_part(4, 4)),
        ("E mid", gather_e.middle),
        ("A z", lambda: (strips_ae.along_z(far_term(0)), strips_ar.along_z(far_term(1)))),
        ("load acts", loads[6].wait),
        ("turn 0", lambda: turn(0, 3)),
        ("E near 1", gather_e.near_one),
        ("R near", gather_r.near),
        ("E fwd 0", lambda: gather_e.forward(0)),
        ("E near 2", gather_e.near_two),
        ("turn 1", lambda: turn(3, 3)),
        ("E fwd 1", lambda: gather_e.forward(-1, -3)),
        ("E fwd 2", lambda: gather_e.forward(-2)),
        ("GE large", scatter_e.large),
        ("GE side", scatter_e.aside),
        ("A mid", lambda: (strips_ae.middle(), strips_ar.middle())),
        ("turn 2", lambda: turn(6, 2)),
        ("E finish", gather_e.finish),
        ("R step 1", lambda: gather_r.step(1)),
        ("E arrived", gather_e.arrived),
        ("hidden", hidden),
        ("GE forward", scatter_e.forward),
        ("GR tiles 0", lambda: gr_part(0, 4)),
        ("GR tiles 1", lambda: gr_part(4, 2)),
        ("GR tiles 2", lambda: gr_part(6, 2)),
        ("R step 2", lambda: gather_r.step(2)),
        ("GR large", scatter_r.large),
        ("GE mid", scatter_e.middle),
        ("GR side", scatter_r.aside),
        ("GR forward", scatter_r.forward),
        ("R step 3", lambda: gather_r.step(3)),
        ("GR mid", scatter_r.middle),
        ("GE z", scatter_e.along_z),
        ("GR z", scatter_r.along_z),
        ("R finish", gather_r.finish),
        ("GE result", lambda: result(0, scatter_e, norms_e, strips_ge)),
        ("R arrived", gather_r.arrived),
        ("A arrived", lambda: (strips_ae.arrived(), strips_ar.arrived())),
        ("GR result", lambda: result(1, scatter_r, norms_r, strips_gr)),
        ("norm e", lambda: norm_step(norms_e)),
        ("gE mid", strips_ge.middle),
        ("gi", lambda: lax.fori_loop(0, tiles, gi_tile, 0)),
        ("norm r", lambda: norm_step(norms_r)),
        ("gR mid", strips_gr.middle),
        ("E update", lambda: update(0, ne, norms_e, strips_ge, gather_ne)),
        ("R update", lambda: update(1, nr, norms_r, strips_gr, gather_nr)),
        ("NE fwd 0", lambda: gather_ne.forward(0, -1, -3, -2)),
        ("NR fwd", lambda: gather_nr.forward(0, -1, -3, -2)),
        ("NE finish", gather_ne.finish),
        ("NR finish", gather_nr.finish),
        ("NE arrived", gather_ne.arrived),
        ("NR arrived", gather_nr.arrived),
    ]
    for name, step in program:
        with scope(name.replace(" ", "_")):
            step()
    with scope("drain"):
        for unit in (
            gather_e, gather_r, gather_ne, gather_nr, scatter_e, scatter_r,
            strips_ae, strips_ar, strips_ge, strips_gr,
        ):
            unit.unit.wait()
        norms_e.sent()
        norms_r.sent()
    assert (net.units, net.used) == (SENDS, RECVS)


def write_out(gi, small, ne, nr, gi_h, nmr_h, nme_h, nvr_h, nve_h, wr_h, we_h, sem):
    copies = [
        pltpu.make_async_copy(src, dst, sem.at[i])
        for i, (src, dst) in enumerate(
            (
                (gi, gi_h),
                (ne, we_h),
                (nr, wr_h),
                (small.at[0], nme_h),
                (small.at[1], nve_h),
                (small.at[2], nmr_h),
                (small.at[3], nvr_h),
            )
        )
    ]
    for copy in copies:
        copy.start()
    for copy in copies:
        copy.wait()


def shards(acts, hid, go, mr, me_, vr, ve):
    rows, channels = acts.shape
    middle = hid.shape[1]
    half = middle // 2
    own = mr.shape
    whole = (NZ, NY, NK * NX, BLK, middle)
    scatter = (
        pltpu.VMEM((2, NK, 4, 4, NZ, BLK, half), BF16),
        pltpu.VMEM((2, 4, 4, NZ, BLK, half), BF16),
        pltpu.VMEM((2, 4, 4, NZ, BLK, half), BF16),
        pltpu.VMEM((2, 4, NZ, BLK, half), BF16),
        pltpu.VMEM((2, 4, NZ, BLK, half), BF16),
        pltpu.VMEM((2, 2, 4, NZ, BLK, half), BF16),
        pltpu.VMEM((2, 4, NZ, BLK, half), BF16),
        pltpu.VMEM((2, 3, NZ, BLK, half), BF16),
        pltpu.VMEM((NZ, BLK, middle), BF16),
        pltpu.VMEM((NZ - 1, BLK, middle), BF16),
    )
    norms = tuple(pltpu.VMEM((n, 1, 128), F32) for n in (NZ, NY * NX * NK, 40))
    in_hbm = pl.BlockSpec(memory_space=pltpu.HBM)
    vmem = pl.BlockSpec(memory_space=pltpu.VMEM)
    args = [pltpu.with_memory_space_constraint(a, pltpu.HBM) for a in (acts, hid, go, mr, me_, vr, ve)]
    results = pl.pallas_call(
        kernel,
        out_shape=(
            pltpu.VMEM((rows, channels), BF16),
            pltpu.VMEM((4, *own), F32),
            pltpu.VMEM(whole, BF16),
            pltpu.VMEM(whole, BF16),
        ),
        in_specs=[in_hbm] * 7,
        out_specs=(vmem,) * 4,
        scratch_shapes=[
            pltpu.VMEM((rows, channels), BF16),
            pltpu.VMEM((rows, middle), BF16),
            pltpu.VMEM((rows, channels), BF16),
            pltpu.VMEM((4, *own), F32),
            pltpu.VMEM((rows, middle), BF16),
            pltpu.VMEM((rows, middle), F32),
            pltpu.VMEM(whole, BF16),
            pltpu.VMEM(whole, BF16),
            pltpu.VMEM((channels, middle), BF16),
            pltpu.VMEM((2, *own), F32),
            pltpu.VMEM((2, NZ, BLK, middle), BF16),
            pltpu.VMEM((2, 2, 4, NZ, BLK, half), BF16),
            pltpu.VMEM((2, NZ, BLK, middle), BF16),
            pltpu.VMEM((2, 2, 4, NZ, BLK, half), BF16),
            pltpu.VMEM((channels, rows), BF16),
            scatter,
            scatter,
            norms,
            norms,
            pltpu.SemaphoreType.DMA((SENDS,)),
            pltpu.SemaphoreType.DMA((RECVS,)),
            pltpu.SemaphoreType.DMA((7,)),
            pltpu.VMEM((512, BLK, half), BF16),
        ],
        compiler_params=pltpu.CompilerParams(
            collective_id=0, has_side_effects=True, vmem_limit_bytes=44 * 1024 * 1024
        ),
    )(*args)
    out = pl.pallas_call(
        write_out,
        out_shape=(
            jax.ShapeDtypeStruct((rows, channels), BF16),
            jax.ShapeDtypeStruct(own, F32),
            jax.ShapeDtypeStruct(own, F32),
            jax.ShapeDtypeStruct(own, F32),
            jax.ShapeDtypeStruct(own, F32),
            jax.ShapeDtypeStruct(whole, BF16),
            jax.ShapeDtypeStruct(whole, BF16),
        ),
        in_specs=[vmem] * 4,
        out_specs=(in_hbm,) * 7,
        scratch_shapes=[pltpu.SemaphoreType.DMA((7,))],
        compiler_params=pltpu.CompilerParams(vmem_limit_bytes=4 * 1024 * 1024),
    )(*results)
    flat = (channels, middle)
    return (*out[:5], out[5].reshape(flat), out[6].reshape(flat))


def solution(mesh):
    split = P(ROWS_SPLIT, None)
    return jax.shard_map(
        shards,
        mesh=mesh,
        in_specs=(split,) * 7,
        out_specs=(split,) * 5 + (P(), P()),
        check_vma=False,
    )
```

```python
import jax
import jax.numpy as jnp
from jax import lax
from jax.experimental import pallas as pl
from jax.experimental.pallas import tpu as pltpu
from jax.sharding import PartitionSpec as P

MESH = pl.DeviceIdType.MESH
BF16 = jnp.bfloat16
F32 = jnp.float32
ROWS_SPLIT = ("gx", "gy", "gz")
NZ, NY, NX, NK = 8, 4, 4, 2
BLK = 8
PIECES = 1
FAR_FIRST = (4, 3, 5, 2, 6, 1, 7)
STRIPS = (2, 1, 3, 0)
PLANE = [(jy, jx) for jy in (2, 1, 3, 0) for jx in (2, 1, 3, 0)][:-1]
SENDS = 12
RECVS = 117
MID_ORDER = (1, 3, 2)


class Group:
    def __init__(self, net, sem):
        self.net, self.sem, self.bytes = net, sem, 0

    def wait(self):
        self.net.wait(self.sem, self.bytes)


class Net:
    def __init__(self, send, recv, spare):
        self.send, self.recv, self.spare = send, recv, spare
        self.used = self.units = 0

    def unit(self):
        self.units += 1
        return Group(self, self.send.at[self.units - 1])

    def group(self):
        self.used += 1
        return Group(self, self.recv.at[self.used - 1])

    def put(self, src, dst, peer, unit, group):
        size = src.dtype.itemsize
        for extent in src.shape:
            size *= extent
        unit.bytes += size
        group.bytes += size
        pltpu.make_async_remote_copy(
            src_ref=src,
            dst_ref=dst,
            send_sem=unit.sem,
            recv_sem=group.sem,
            device_id=peer,
            device_id_type=MESH,
        ).start()

    def wait(self, sem, size):
        blocks, rest = divmod(size, 4096)
        assert rest == 0
        ref = self.spare.at[pl.ds(0, blocks)]
        pltpu.make_async_copy(ref, ref, sem).wait()


class Place:
    def __init__(self):
        self.z = lax.axis_index("gx")
        gy = lax.axis_index("gy")
        self.y = gy // 2
        self.k = gy % 2
        self.x = lax.axis_index("gz")
        self.gy = gy
        self.kx = self.k * NX + self.x
        self.d = 1 - 2 * self.k

    def zp(self, j):
        return {"gx": (self.z + j + NZ) % NZ}

    def plane(self, jy, jk, jx):
        y = (self.y + jy) % NY
        return {"gy": y * NK + (self.k + jk) % NK, "gz": (self.x + jx) % NX}

    def yp(self, j):
        return {"gy": ((self.y + j + NY) % NY) * 2 + self.k}

    def xp(self, j):
        return {"gz": (self.x + j + NX) % NX}

    def other(self):
        return {"gy": self.gy + 1 - 2 * self.k}


class Gather:
    def __init__(self, net, me, w):
        self.net, self.me, self.w = net, me, w
        half = w.shape[-1] // 2
        self.parts = (pl.ds(0, half), pl.ds(half, half))
        self.unit = net.unit()
        self.cores = net.group()
        self.ahead = ({}, {})
        self.side = [net.group() for part in range(2)]
        self.far = [[net.group(), net.group()] for part in range(2)]

    def put(self, ref, peer, group):
        self.net.put(ref, ref, peer, self.unit, group)

    def along_z(self):
        me = self.me
        ref = self.w.at[me.z, me.y, me.kx]
        self.zs = self.net.group()
        for j in FAR_FIRST:
            self.put(ref, me.zp(j), self.zs)

    def at(self, part, large, mid):
        me = self.me
        x = (me.x + (large if part == 0 else mid) + NX) % NX
        y = (me.y + (mid if part == 0 else large) + NY) % NY
        return self.w.at[:, y, me.k * NX + x, :, self.parts[part]]

    def slab(self, part, off):
        me = self.me
        if part == 0:
            x = (me.x + off + NX) % NX
            return self.w.at[:, :, me.k * NX + x, :, self.parts[0]]
        y = (me.y + off + NY) % NY
        return self.w.at[:, y, pl.ds(me.k * NX, NX), :, self.parts[1]]

    def peer(self, part, off):
        return self.me.xp(off) if part == 0 else self.me.yp(off)

    def core(self, ref):
        self.put(ref, self.me.other(), self.cores)

    def across(self, part, off):
        me = self.me
        return me.plane(0, 1, off + NX) if part == 0 else me.plane(off + NY, 1, 0)

    def near(self, part, mid):
        d = self.me.d
        self.ahead[part][mid] = self.net.group()
        self.put(self.at(part, 0, mid), self.peer(part, d), self.ahead[part][mid])
        self.put(self.at(part, 0, mid), self.peer(part, -d), self.side[part])

    def middle(self):
        self.zs.wait()
        self.mids = [{j: self.net.group() for j in MID_ORDER} for part in range(2)]
        for j in MID_ORDER:
            for part in range(2):
                self.put(self.at(part, 0, 0), self.peer(1 - part, j), self.mids[part][j])
        for part in range(2):
            self.near(part, 0)

    def near_one(self):
        for j in (1, 3):
            for part in range(2):
                self.mids[part][j].wait()
                self.near(part, -j)

    def near_two(self):
        for part in range(2):
            self.mids[part][2].wait()
            self.near(part, -2)
        for part in range(2):
            self.core(self.slab(part, 0))

    def near_all(self):
        for mid in (0, -1, -3, -2):
            for part in range(2):
                self.near(part, mid)
        for part in range(2):
            self.core(self.slab(part, 0))

    def forward(self, *mids):
        d = self.me.d
        for mid in mids:
            for part in range(2):
                self.ahead[part][mid].wait()
                ref = self.at(part, -d, mid)
                self.put(ref, self.peer(part, d), self.far[part][1 if mid == -2 else 0])
                if mid == -2:
                    self.put(ref, self.across(part, d), self.cores)
        if -2 in mids:
            for part in range(2):
                self.core(self.slab(part, -d))

    def finish(self):
        d = self.me.d
        for part in range(2):
            self.side[part].wait()
            self.core(self.slab(part, d))
        for part in range(2):
            self.far[part][0].wait()
            for mid in (0, -1, -3):
                self.core(self.at(part, 2, mid))
        for part in range(2):
            self.far[part][1].wait()

    def arrived(self):
        self.cores.wait()


class GatherRound:
    def __init__(self, net, me, w):
        self.net, self.me, self.w = net, me, w
        self.unit = net.unit()
        self.blocks, self.cores, self.last = net.group(), net.group(), net.group()
        self.up = [net.group() for step in range(3)]
        self.down = [net.group() for step in range(3)]

    def put(self, ref, peer, group):
        self.net.put(ref, ref, peer, self.unit, group)

    def plane(self):
        me = self.me
        ref = self.w.at[me.z, me.y, me.kx]
        for jy, jx in PLANE:
            self.put(ref, me.plane(jy, 0, jx), self.blocks)

    def slab(self, off):
        me = self.me
        return self.w.at[(me.z + off + NZ) % NZ, :, pl.ds(me.k * NX, NX)]

    def core(self, off):
        self.put(self.slab(off), self.me.other(), self.cores)

    def near(self):
        self.blocks.wait()
        self.put(self.slab(0), self.me.zp(1), self.up[0])
        self.put(self.slab(0), self.me.zp(-1), self.down[0])
        self.core(0)

    def step(self, i):
        self.up[i - 1].wait()
        if i < 3:
            self.put(self.slab(-i), self.me.zp(1), self.up[i])
        self.down[i - 1].wait()
        if i < 3:
            self.put(self.slab(i), self.me.zp(-1), self.down[i])
        else:
            d = self.me.d
            self.put(self.slab(-3 * d), self.me.zp(d), self.last)
        self.core(-i)
        self.core(i)

    def finish(self):
        self.last.wait()
        self.core(4)

    def arrived(self):
        self.cores.wait()


class Strips:
    def __init__(self, net, me, zb, m):
        self.net, self.me, self.zb, self.m = net, me, zb, m
        self.unit, self.zs, self.mids = net.unit(), net.group(), net.group()

    def along_z(self, block):
        me = self.me
        self.zb[me.z] = block
        ref = self.zb.at[me.z]
        for j in FAR_FIRST:
            self.net.put(ref, ref, me.zp(j), self.unit, self.zs)

    def middle(self):
        me = self.me
        half = self.m.shape[-1]
        self.zs.wait()
        for j in (2, 1, 3):
            for part, peer, own in ((0, me.yp, me.y), (1, me.xp, me.x)):
                src = self.zb.at[:, :, pl.ds(part * half, half)]
                self.net.put(src, self.m.at[part, own], peer(j), self.unit, self.mids)
        for part, own in ((0, me.y), (1, me.x)):
            self.m[part, own] = self.zb[:, :, pl.ds(part * half, half)]

    def arrived(self):
        self.mids.wait()


class Scatter:
    def __init__(self, net, me, refs):
        self.net, self.me = net, me
        (self.p, self.c, self.s, self.f, self.t, self.r, self.a, self.m, self.b, self.q) = refs
        self.unit = net.unit()
        self.cs = net.group()
        self.near = [[net.group() for mid in range(4)] for part in range(2)]
        self.far = [[net.group() for mid in range(4)] for part in range(2)]
        self.side = [net.group() for part in range(2)]
        self.mids = [net.group() for part in range(2)]
        self.zs = net.group()

    def put(self, src, dst, peer, group):
        self.net.put(src, dst, peer, self.unit, group)

    def tile(self, t, value):
        half = value.shape[1] // 2
        for y in range(NY):
            for k in range(NK):
                for x in range(NX):
                    at = ((y * NK + k) * NX + x) * BLK
                    rows = value[at : at + BLK]
                    self.p[0, k, x, y, t] = rows[:, :half].astype(BF16)
                    self.p[1, k, y, x, t] = rows[:, half:].astype(BF16)

    def cores(self, first, count):
        me = self.me
        zs = pl.ds(first, count)
        for part in range(2):
            self.put(
                self.p.at[part, 1 - me.k, :, :, zs],
                self.c.at[part, :, :, zs],
                me.other(),
                self.cs,
            )

    def peer(self, part, off):
        return self.me.xp(off) if part == 0 else self.me.yp(off)

    def index(self, part, off):
        return (self.me.x + off + NX) % NX if part == 0 else (self.me.y + off + NY) % NY

    def joined(self, part, off, mid):
        at, i = self.index(part, off), self.index(1 - part, mid)
        total = self.p[part, self.me.k, at, i].astype(F32) + self.c[part, at, i].astype(F32)
        self.s[part, at, i] = total.astype(BF16)
        return self.s.at[part, at, i]

    def large(self):
        d = self.me.d
        self.cs.wait()
        for mid in STRIPS:
            for part in range(2):
                dst = self.f.at[part, self.index(1 - part, mid)]
                src = self.joined(part, 2, mid)
                self.put(src, dst, self.peer(part, d), self.near[part][mid])

    def aside(self):
        d = self.me.d
        for mid in STRIPS:
            for part in range(2):
                dst = self.r.at[part, 0, self.index(1 - part, mid)]
                src = self.joined(part, -d, mid)
                self.put(src, dst, self.peer(part, -d), self.side[part])
        for mid in STRIPS:
            for part in range(2):
                self.joined(part, d, mid)
                self.joined(part, 0, mid)

    def forward(self, *mids):
        d = self.me.d
        for mid in mids:
            for part in range(2):
                self.near[part][mid].wait()
                i = self.index(1 - part, mid)
                total = self.s[part, self.index(part, d), i].astype(F32)
                total = total + self.f[part, i].astype(F32)
                self.t[part, i] = total.astype(BF16)
                dst = self.r.at[part, 1, i]
                self.put(self.t.at[part, i], dst, self.peer(part, d), self.far[part][mid])

    def middle(self, *mids):
        if mids[0] == STRIPS[0]:
            for part in range(2):
                self.side[part].wait()
        for mid in mids:
            for part in range(2):
                self.far[part][mid].wait()
                i = self.index(1 - part, mid)
                total = self.s[part, self.index(part, 0), i].astype(F32)
                total = total + self.r[part, 0, i].astype(F32)
                total = total + self.r[part, 1, i].astype(F32)
                self.a[part, i] = total.astype(BF16)
                if mid:
                    dst = self.m.at[part, mid - 1]
                    self.put(self.a.at[part, i], dst, self.peer(1 - part, mid), self.mids[part])

    def along_z(self):
        me = self.me
        for part in range(2):
            self.mids[part].wait()
            at = self.index(1 - part, 0)
            total = self.a[part, at].astype(F32)
            for j in range(3):
                total = total + self.m[part, j].astype(F32)
            half = total.shape[-1]
            self.b[:, :, pl.ds(part * half, half)] = total.astype(BF16)
        for j in FAR_FIRST:
            self.put(self.b.at[(me.z + j) % NZ], self.q.at[j - 1], me.zp(j), self.zs)

    def result(self):
        self.zs.wait()
        total = self.b[self.me.z].astype(F32)
        for j in range(7):
            total = total + self.q[j].astype(F32)
        return total


class Norms:
    def __init__(self, net, me, refs):
        self.net, self.me, self.refs = net, me, refs
        self.unit = net.unit()
        self.groups = [net.group() for axis in range(2)]

    def start(self, axis, row):
        me = self.me
        ref = self.refs[axis]
        own = me.gy * NX + me.x if axis else me.z
        ref[own] = row
        peers = [me.zp(j) for j in FAR_FIRST]
        if axis:
            peers = [me.plane(jy, 1, jx) for jy, jx in PLANE]
            peers += [me.plane(jy, 0, jx) for jy, jx in PLANE] + [me.other()]
        for peer in peers:
            self.net.put(ref.at[own], ref.at[own], peer, self.unit, self.groups[axis])

    def finish(self, axis):
        ref = self.refs[axis]
        self.wait(self.groups[axis].sem, ref.shape[0] - 1)
        total = ref[0]
        for i in range(1, ref.shape[0]):
            total = total + ref[i]
        return total

    def wait(self, sem, count):
        ref = self.refs[2].at[pl.ds(0, count)]
        pltpu.make_async_copy(ref, ref, sem).wait()

    def sent(self):
        self.wait(self.unit.sem, NZ + NY * NX * NK - 2)


def fold(sq):
    lanes = sq[:, 0:128]
    for i in range(1, sq.shape[1] // 128):
        lanes = lanes + sq[:, 128 * i : 128 * (i + 1)]
    row = jnp.sum(lanes, axis=0, keepdims=True)
    return row + pltpu.roll(row, 64, 1)


def low_lanes():
    return lax.broadcasted_iota(jnp.int32, (1, 128), 1) < 64


def stat_row(w, g):
    return jnp.where(low_lanes(), fold(w * w), fold(g * g))


def trust_of(row):
    wsquare = jnp.sum(jnp.where(low_lanes(), row, 0.0), axis=1, keepdims=True)
    gsquare = jnp.sum(jnp.where(low_lanes(), 0.0, row), axis=1, keepdims=True)
    wnorm = jnp.sqrt(wsquare)
    gnorm = jnp.sqrt(gsquare)
    return wnorm / (gnorm + 5e-05 * wnorm)


def updated(master, grads, velocity, trust):
    new_velocity = 0.9 * velocity + trust * (grads + 5e-05 * master)
    new_master = master - 0.1 * new_velocity
    return new_master, new_velocity


def kernel(
    acts_h, hid_h, go_h, mr_h, me_h, vr_h, ve_h,
    gi, smallout, ne, nr,
    acts, hid, go, small, gh, acc,
    we, wr, flat, g_kept, az, am, gz, gm, turned, ge_refs, gr_refs, nz_e, nz_r,
    send, recv, load, spare,
):
    scope = jax.named_scope
    me = Place()
    net = Net(send, recv, spare)
    channels = go.shape[1]
    middle = hid.shape[1]
    half = middle // 2
    inv_c = 1.0 / float(channels) ** 0.5
    inv_m = 1.0 / float(middle) ** 0.5

    loads = [
        pltpu.make_async_copy(src, dst, load.at[i])
        for i, (src, dst) in enumerate(
            (
                (me_h, small.at[0]),
                (mr_h, small.at[1]),
                (vr_h, small.at[3]),
                (ve_h, small.at[2]),
                (go_h, go),
                (hid_h, hid),
                (acts_h, acts),
            )
        )
    ]
    for copy in loads:
        copy.start()

    barrier = pltpu.get_barrier_semaphore()
    peers = [me.zp(j) for j in FAR_FIRST] + [me.other()]
    peers += [me.plane(jy, jk, jx) for jk in range(NK) for jy, jx in PLANE]
    for peer in peers:
        pl.semaphore_signal(barrier, inc=1, device_id=peer, device_id_type=MESH)

    for copy in loads[:4]:
        copy.wait()
    we[me.z, me.y, me.kx] = small[0].astype(BF16)
    wr[me.z, me.y, me.kx] = small[1].astype(BF16)
    with scope("barrier"):
        pl.semaphore_wait(barrier, len(peers))

    gather_e = Gather(net, me, we)
    gather_r = GatherRound(net, me, wr)
    gather_ne = Gather(net, me, ne)
    gather_nr = Gather(net, me, nr)
    scatter_e = Scatter(net, me, ge_refs)
    scatter_r = Scatter(net, me, gr_refs)
    norms_e = Norms(net, me, nz_e)
    norms_r = Norms(net, me, nz_r)
    strips_ae = Strips(net, me, az.at[0], am.at[0])
    strips_ar = Strips(net, me, az.at[1], am.at[1])
    strips_ge = Strips(net, me, gz.at[0], gm.at[0])
    strips_gr = Strips(net, me, gz.at[1], gm.at[1])
    tiles = channels // 256

    def tile_cols(t):
        return pl.ds(pl.multiple_of(t * 256, 256), 256)

    def natural(w, t):
        block = w[t].reshape(NY * NK * NX, BLK, middle)
        return block.astype(F32).reshape(256, middle).astype(BF16)

    def ge_tile(t, carry):
        value = lax.dot_general(
            go[:, tile_cols(t)], hid[...], (((0,), (0,)), ((), ())), preferred_element_type=F32
        )
        scatter_e.tile(t, value * inv_m)
        return carry

    def gr_tile(t, carry):
        value = jnp.dot(turned[tile_cols(t), :], gh[...], preferred_element_type=F32)
        scatter_r.tile(t, value * inv_c)
        return carry

    def flatten(t, carry):
        flat[tile_cols(t), :] = natural(we, t)
        return carry

    def gi_tile(t, carry):
        cols = tile_cols(t)
        back = lax.dot_general(
            gh[...], natural(wr, t), (((1,), (1,)), ((), ())), preferred_element_type=F32
        )
        gi[:, cols] = (go[:, cols].astype(F32) + back * inv_c).astype(BF16)
        return carry

    def far_term(i):
        return (small[i] - 0.09 * small[i + 2]).astype(BF16)

    def result(i, scatter, norms, strips):
        g = scatter.result()
        g_kept[i] = g
        norms.start(0, stat_row(small[i], g))
        strips.along_z((g + 5e-05 * small[i]).astype(BF16))

    def norm_step(norms):
        norms.start(1, norms.finish(0))

    def update(i, out, norms, strips, gather):
        trust = trust_of(norms.finish(1))
        strips.arrived()
        step = jnp.broadcast_to(0.1 * trust, (BLK, half))

        def fill(at, carry):
            for z in range(NZ):
                for part in range(2):
                    block = am[i, part, at, z].astype(F32) - step * gm[i, part, at, z].astype(F32)
                    if part == 0:
                        out[z, at, me.kx, :, pl.ds(0, half)] = block.astype(BF16)
                    else:
                        out[z, me.y, me.k * NX + at, :, pl.ds(half, half)] = block.astype(BF16)
            return carry

        lax.fori_loop(0, 4, fill, 0)
        gather.near_all()
        new_master, new_velocity = updated(small[i], g_kept[i], small[i + 2], trust)
        smallout[2 * i] = new_master
        smallout[2 * i + 1] = new_velocity

    def turn(first, count):
        def one(t, carry):
            turned[tile_cols(t), :] = acts[:, tile_cols(t)].T
            return carry

        lax.fori_loop(first, first + count, one, 0)

    def ge_part(first, count):
        lax.fori_loop(first, first + count, ge_tile, 0)
        scatter_e.cores(first, count)

    def gr_part(first, count):
        lax.fori_loop(first, first + count, gr_tile, 0, unroll=True)
        scatter_r.cores(first, count)

    def hidden():
        lax.fori_loop(0, tiles, flatten, 0)
        acc[...] = jnp.dot(go[...], flat[...], preferred_element_type=F32)
        gh[...] = jnp.where(hid[...].astype(F32) > 0, acc[...] * inv_m, 0.0).astype(BF16)

    program = [
        ("E z", gather_e.along_z),
        ("R plane", gather_r.plane),
        ("load go", loads[4].wait),
        ("load hid", loads[5].wait),
        ("GE tiles 0", lambda: ge_part(0, 4)),
        ("GE tiles 1", lambda: ge_part(4, 4)),
        ("E mid", gather_e.middle),
        ("A z", lambda: (strips_ae.along_z(far_term(0)), strips_ar.along_z(far_term(1)))),
        ("load acts", loads[6].wait),
        ("turn 0", lambda: turn(0, 3)),
        ("E near 1", gather_e.near_one),
        ("R near", gather_r.near),
        ("E fwd 0", lambda: gather_e.forward(0)),
        ("E near 2", gather_e.near_two),
        ("turn 1", lambda: turn(3, 3)),
        ("E fwd 1", lambda: gather_e.forward(-1, -3)),
        ("E fwd 2", lambda: gather_e.forward(-2)),
        ("GE large", scatter_e.large),
        ("GE side", scatter_e.aside),
        ("turn 2", lambda: turn(6, 2)),
        ("E finish", gather_e.finish),
        ("R step 1", lambda: gather_r.step(1)),
        ("E arrived", gather_e.arrived),
        ("hidden", hidden),
        ("GE forward", lambda: scatter_e.forward(*STRIPS)),
        ("GR tiles 0", lambda: gr_part(0, 4)),
        ("GR tiles 1", lambda: gr_part(4, 2)),
        ("GR tiles 2", lambda: gr_part(6, 2)),
        ("R step 2", lambda: gather_r.step(2)),
        ("GR large", scatter_r.large),
        ("GE mid", lambda: scatter_e.middle(*STRIPS)),
        ("GR side", scatter_r.aside),
        ("GR fwd 0", lambda: scatter_r.forward(2, 1)),
        ("GR fwd 1", lambda: scatter_r.forward(3, 0)),
        ("R step 3", lambda: gather_r.step(3)),
        ("GR mid 0", lambda: scatter_r.middle(2, 1)),
        ("GE z", scatter_e.along_z),
        ("GR mid 1", lambda: scatter_r.middle(3, 0)),
        ("GR z", scatter_r.along_z),
        ("R finish", gather_r.finish),
        ("A mid", lambda: (strips_ae.middle(), strips_ar.middle())),
        ("GE result", lambda: result(0, scatter_e, norms_e, strips_ge)),
        ("GR result", lambda: result(1, scatter_r, norms_r, strips_gr)),
        ("norm e", lambda: norm_step(norms_e)),
        ("gE mid", strips_ge.middle),
        ("R arrived", gather_r.arrived),
        ("gi", lambda: lax.fori_loop(0, tiles, gi_tile, 0, unroll=2)),
        ("A arrived", lambda: (strips_ae.arrived(), strips_ar.arrived())),
        ("norm r", lambda: norm_step(norms_r)),
        ("gR mid", strips_gr.middle),
        ("E update", lambda: update(0, ne, norms_e, strips_ge, gather_ne)),
        ("R update", lambda: update(1, nr, norms_r, strips_gr, gather_nr)),
        ("NE fwd 0", lambda: gather_ne.forward(0, -1)),
        ("NE fwd 1", lambda: gather_ne.forward(-3, -2)),
        ("NR fwd", lambda: gather_nr.forward(0, -1, -3, -2)),
        ("NE finish", gather_ne.finish),
        ("NR finish", gather_nr.finish),
        ("NE arrived", gather_ne.arrived),
        ("NR arrived", gather_nr.arrived),
    ]
    for name, step in program:
        with scope(name.replace(" ", "_")):
            step()
    with scope("drain"):
        for unit in (
            gather_e, gather_r, gather_ne, gather_nr, scatter_e, scatter_r,
            strips_ae, strips_ar, strips_ge, strips_gr,
        ):
            unit.unit.wait()
        norms_e.sent()
        norms_r.sent()
    assert (net.units, net.used) == (SENDS, RECVS)


def write_out(gi, small, ne, nr, gi_h, nmr_h, nme_h, nvr_h, nve_h, wr_h, we_h, sem):
    pairs = [(small.at[i], ref) for i, ref in enumerate((nme_h, nve_h, nmr_h, nvr_h))]
    for i in range(PIECES):
        zs = pl.ds(i * (NZ // PIECES), NZ // PIECES)
        wide = gi.shape[1] // PIECES
        cols = pl.ds(i * wide, wide)
        pairs += [(nr.at[zs], wr_h.at[zs]), (ne.at[zs], we_h.at[zs])]
        pairs += [(gi.at[:, cols], gi_h.at[:, cols])]
    copies = [pltpu.make_async_copy(src, dst, sem.at[i]) for i, (src, dst) in enumerate(pairs)]
    for copy in copies:
        copy.start()
    for copy in copies:
        copy.wait()


def shards(acts, hid, go, mr, me_, vr, ve):
    rows, channels = acts.shape
    middle = hid.shape[1]
    half = middle // 2
    own = mr.shape
    whole = (NZ, NY, NK * NX, BLK, middle)
    scatter = (
        pltpu.VMEM((2, NK, 4, 4, NZ, BLK, half), BF16),
        pltpu.VMEM((2, 4, 4, NZ, BLK, half), BF16),
        pltpu.VMEM((2, 4, 4, NZ, BLK, half), BF16),
        pltpu.VMEM((2, 4, NZ, BLK, half), BF16),
        pltpu.VMEM((2, 4, NZ, BLK, half), BF16),
        pltpu.VMEM((2, 2, 4, NZ, BLK, half), BF16),
        pltpu.VMEM((2, 4, NZ, BLK, half), BF16),
        pltpu.VMEM((2, 3, NZ, BLK, half), BF16),
        pltpu.VMEM((NZ, BLK, middle), BF16),
        pltpu.VMEM((NZ - 1, BLK, middle), BF16),
    )
    norms = tuple(pltpu.VMEM((n, 1, 128), F32) for n in (NZ, NY * NX * NK, 40))
    in_hbm = pl.BlockSpec(memory_space=pltpu.HBM)
    vmem = pl.BlockSpec(memory_space=pltpu.VMEM)
    args = [pltpu.with_memory_space_constraint(a, pltpu.HBM) for a in (acts, hid, go, mr, me_, vr, ve)]
    results = pl.pallas_call(
        kernel,
        out_shape=(
            pltpu.VMEM((rows, channels), BF16),
            pltpu.VMEM((4, *own), F32),
            pltpu.VMEM(whole, BF16),
            pltpu.VMEM(whole, BF16),
        ),
        in_specs=[in_hbm] * 7,
        out_specs=(vmem,) * 4,
        scratch_shapes=[
            pltpu.VMEM((rows, channels), BF16),
            pltpu.VMEM((rows, middle), BF16),
            pltpu.VMEM((rows, channels), BF16),
            pltpu.VMEM((4, *own), F32),
            pltpu.VMEM((rows, middle), BF16),
            pltpu.VMEM((rows, middle), F32),
            pltpu.VMEM(whole, BF16),
            pltpu.VMEM(whole, BF16),
            pltpu.VMEM((channels, middle), BF16),
            pltpu.VMEM((2, *own), F32),
            pltpu.VMEM((2, NZ, BLK, middle), BF16),
            pltpu.VMEM((2, 2, 4, NZ, BLK, half), BF16),
            pltpu.VMEM((2, NZ, BLK, middle), BF16),
            pltpu.VMEM((2, 2, 4, NZ, BLK, half), BF16),
            pltpu.VMEM((channels, rows), BF16),
            scatter,
            scatter,
            norms,
            norms,
            pltpu.SemaphoreType.DMA((SENDS,)),
            pltpu.SemaphoreType.DMA((RECVS,)),
            pltpu.SemaphoreType.DMA((7,)),
            pltpu.VMEM((512, BLK, half), BF16),
        ],
        compiler_params=pltpu.CompilerParams(
            collective_id=0, has_side_effects=True, vmem_limit_bytes=44 * 1024 * 1024
        ),
    )(*args)
    out = pl.pallas_call(
        write_out,
        out_shape=(
            jax.ShapeDtypeStruct((rows, channels), BF16),
            jax.ShapeDtypeStruct(own, F32),
            jax.ShapeDtypeStruct(own, F32),
            jax.ShapeDtypeStruct(own, F32),
            jax.ShapeDtypeStruct(own, F32),
            jax.ShapeDtypeStruct(whole, BF16),
            jax.ShapeDtypeStruct(whole, BF16),
        ),
        in_specs=[vmem] * 4,
        out_specs=(in_hbm,) * 7,
        scratch_shapes=[pltpu.SemaphoreType.DMA((4 + 3 * PIECES,))],
        compiler_params=pltpu.CompilerParams(vmem_limit_bytes=4 * 1024 * 1024),
    )(*results)
    flat = (channels, middle)
    return (*out[:5], out[5].reshape(flat), out[6].reshape(flat))


def solution(mesh):
    split = P(ROWS_SPLIT, None)
    return jax.shard_map(
        shards,
        mesh=mesh,
        in_specs=(split,) * 7,
        out_specs=(split,) * 5 + (P(), P()),
        check_vma=False,
    )
```
